256 devices in a mesh: member: 8 (over y_lo, x), grid: 32 (over z, y_hi, core).
Axes of the slice: x: 4, y: 4 (y_hi: 2, y_lo: 2; y = y_hi * 2 + y_lo), z: 8, core: 2. Of those that a mesh axis runs over, the one named last changes fastest.
Arguments:
- prior_ensemble: bfloat16 [40, 48, 131072], P('member', None, 'grid'), may hold values from -6 to 6
- domain_site_mapping: int32 [32, 8, 512], P(None, None, 'grid'), may hold values from 0 to 4095, as said below
- neighbour_triples: int32 [32, 3, 4096], P('grid', None, 'member'), may hold values from 0 to 159
- stencil_factors: float32 [32, 3, 4096], P('grid', None, 'member'), may hold values from 0.1 to 1
- sparse_node_transforms: float32 [1600, 4096], P(None, 'grid'), may hold values from -0.4 to 1.8
Outputs:
- analysis: bfloat16 [40, 48, 131072], P('member', None, 'grid')
The draws below stay inside these ranges and needn't reach their ends.
Inputs may be any that keep to these rules, and one draw needn't show every extreme that they name: For every model patch h, the entries domain_site_mapping[:, :, h * 16 : (h + 1) * 16] hold every number from 0 to 4095 exactly once.
All inputs are finite; a program needn't handle non-finite values.
Results may differ from the reference program's by a relative error of at most 0.0076.
Values may be sent and summed in bfloat16 or wider, within the bound.
A program may use at most 128 MiB of HBM per device.

```python
import math
import jax
import jax.numpy as jnp
from jax import lax

ENSEMBLE_SIZE = 40
STATE_QUANTITIES = 48
CELLS_DEV = 4096
COARSE_DEV = 128
RIM = 16
PATCHES = 32
GROUPS = 8
COLUMNS = 512
PER_SOURCE = 16
MESH_SITES = 131072
COARSE = 4096


def draw_domain_site_mapping(key, part):
    subkeys = jax.random.split(jax.random.fold_in(key, 11), PATCHES)
    shuffled = jax.vmap(lambda subkey: jax.random.permutation(subkey, CELLS_DEV))(subkeys)
    shuffled = shuffled.reshape(PATCHES, PATCHES, GROUPS, PER_SOURCE)
    return jnp.transpose(shuffled, (1, 2, 0, 3)).reshape(PATCHES, GROUPS, COLUMNS).astype(jnp.int32)


def draw_sparse_node_transforms(key, part):
    first_key = jax.random.fold_in(key, 21)
    second_key = jax.random.fold_in(key, 22)
    scatter_part = jnp.clip(0.12 * jax.random.normal(first_key, (ENSEMBLE_SIZE, ENSEMBLE_SIZE, COARSE), jnp.float32), -0.4, 0.4)
    diagonal_part = jax.random.uniform(second_key, (ENSEMBLE_SIZE, COARSE), jnp.float32, 0.6, 1.4)
    weights = scatter_part + jnp.eye(ENSEMBLE_SIZE, dtype=jnp.float32)[:, :, None] * diagonal_part[:, None, :]
    return weights.reshape(ENSEMBLE_SIZE * ENSEMBLE_SIZE, COARSE).astype(jnp.float32)


def place_ends(drawn, stream_key, smallest, high):
    spot = [jax.random.randint(jax.random.fold_in(stream_key, axis), (), 0, length) for axis, length in enumerate(drawn.shape)]
    widest = drawn.shape.index(max(drawn.shape))
    next_to = spot[:widest] + [(spot[widest] + 1) % drawn.shape[widest]] + spot[widest + 1:]
    return drawn.at[tuple(spot)].set(smallest).at[tuple(next_to)].set(high)


def shard_levels(rng, dims, cuts, low, top_value):
    factor_of = 1.0
    for dim, parts in cuts:
        steps = jax.random.uniform(jax.random.fold_in(jax.random.fold_in(rng, 6), dim), (parts,), jnp.float32, low / len(cuts), top_value / len(cuts))
        factor_of = factor_of * jnp.repeat(jnp.exp(steps), dims[dim] // parts).reshape((-1,) + (1,) * (len(dims) - 1 - dim))
    return factor_of


def scatter_about(stream_key, shape, scale, limit, pieces=(), kind=jnp.bfloat16):
    gain = shard_levels(stream_key, shape, pieces, -0.22, 0.18) if pieces else 1.0
    entries = jax.random.normal(stream_key, shape, jnp.float32) * scale * gain
    return jnp.minimum(jnp.maximum(entries, -limit), limit).astype(kind)


def setup_inputs(seed: int = 0) -> dict:
    seeds = jax.random.split(jax.random.key(seed), 6)
    return {
        "prior_ensemble": scatter_about(seeds[0], (ENSEMBLE_SIZE, STATE_QUANTITIES, MESH_SITES), 1.0, 6.0, ((0, 8), (2, 32))),
        "domain_site_mapping": draw_domain_site_mapping(jax.random.fold_in(seeds[5], 71), 0),
        "neighbour_triples": place_ends(jax.random.randint(seeds[2], (PATCHES, 3, CELLS_DEV), 0, COARSE_DEV + 2 * RIM), jax.random.fold_in(seeds[2], 1), 0, (COARSE_DEV + 2 * RIM) - 1).astype(jnp.int32),
        "stencil_factors": jnp.clip(jnp.exp(math.log(1.0) - 2.3025851 * jax.random.uniform(seeds[3], (PATCHES, 3, CELLS_DEV), jnp.float32) ** shard_levels(seeds[3], (PATCHES, 3, CELLS_DEV), ((0, 32), (2, 8)), -0.2, 0.2)), 0.1, 1.0),
        "sparse_node_transforms": draw_sparse_node_transforms(jax.random.fold_in(seeds[5], 71), 0),
    }


def reference(prior_ensemble, domain_site_mapping, neighbour_triples, stencil_factors, sparse_node_transforms):
    source_base = (jnp.arange(COLUMNS, dtype=jnp.int32) // PER_SOURCE) * CELLS_DEV
    cell_ids = (domain_site_mapping + source_base[None, None, :]).reshape(PATCHES, CELLS_DEV).astype(jnp.int32)

    def one_patch(inputs):
        sites_within_tile, points, raw_share, patch_id = inputs
        arriving_analysis_slots = jnp.take(prior_ensemble, sites_within_tile, axis=2)
        member_mean = jnp.sum(arriving_analysis_slots, axis=0, dtype=jnp.float32) / ENSEMBLE_SIZE
        deviation = (arriving_analysis_slots.astype(jnp.float32) - member_mean[None]).astype(jnp.bfloat16)
        coarse_ids = ((patch_id * COARSE_DEV - RIM + points) % COARSE).astype(jnp.int32)
        shares = raw_share / jnp.sum(raw_share, axis=0, keepdims=True)
        blended = jnp.zeros((ENSEMBLE_SIZE * ENSEMBLE_SIZE, CELLS_DEV), jnp.float32)
        for which in range(3):
            blended = blended + jnp.take(sparse_node_transforms, coarse_ids[which], axis=1) * shares[which][None, :]
        blended = blended.reshape(ENSEMBLE_SIZE, ENSEMBLE_SIZE, CELLS_DEV).astype(jnp.bfloat16)
        result = jnp.einsum('kfc,kjc->jfc', deviation.astype(jnp.float32), blended.astype(jnp.float32)) + member_mean[None]
        return result.astype(jnp.bfloat16)

    patch_list = jnp.arange(PATCHES, dtype=jnp.int32)
    results = lax.map(one_patch, (cell_ids, neighbour_triples, stencil_factors, patch_list))
    ordered = jnp.moveaxis(results, 0, 2).reshape(ENSEMBLE_SIZE, STATE_QUANTITIES, MESH_SITES)
    analysis = jnp.zeros((ENSEMBLE_SIZE, STATE_QUANTITIES, MESH_SITES), jnp.bfloat16)
    analysis = analysis.at[:, :, cell_ids.reshape(-1)].set(ordered)
    return analysis
```

```python
import functools

import jax
import jax.numpy as jnp
from jax import lax
from jax.experimental import pallas as pl
from jax.experimental.pallas import tpu as pltpu
from jax.sharding import PartitionSpec as P

MESH = pl.DeviceIdType.MESH
F32, BF16 = jnp.float32, jnp.bfloat16

MEMBERS = 40
LOCAL = 5
FIELDS = 48
ROWS = LOCAL * FIELDS
PATCH = 4096
BLOCK = 512
GROUPS = 8
POINTS = 128
RIM = 16
PAIRS = 200
HEAD = 16
PACKET = HEAD + 208


def onehot_into(oh_ref, hi_ref, ids):
    hi, lo = ids >> 6, ids & 63
    level = lax.broadcasted_iota(jnp.int32, (64, BLOCK), 0)
    hi_ref[...] = jnp.where(level == hi, 1.0, 0.0).astype(F32)
    low = jnp.where(level == lo, 1.0, 0.0).astype(BF16).reshape(4, 16, BLOCK)
    for h in range(64):
        row = jnp.broadcast_to(hi_ref[h : h + 1, :], (16, BLOCK)).astype(BF16)
        oh_ref[h * 64 : (h + 1) * 64, :] = (low * row[None]).reshape(64, BLOCK)


def kernel(
    prior_ref, ids_ref, pts_ref, fac_ref, trans_ref, out_ref,
    zsend, zrecv, tbuf, rimsend, rimbuf, picked, gathered, mean, dev, weights,
    result, returned, total, oh, hi_ref, spread, spread_rim,
    zs_send, zs_recv, t_send, t_recv, d_sems, rim_send, rim_recv,
    st_send, st_recv, rt_send, rt_recv,
):
    m, g = lax.axis_index("member"), lax.axis_index("grid")
    z, q = g // 4, g % 4
    yh, c = q // 2, q % 2
    rim_end = jnp.logical_or(q == 0, q == 3)
    low_end = q == 3
    rim_member = jnp.where(low_end, (z + 1) % 8, (z + 7) % 8)

    barrier = pltpu.get_barrier_semaphore()

    def greet(member, grid):
        pl.semaphore_signal(barrier, inc=1, device_id=(member, grid), device_id_type=MESH)

    for s in range(1, 8):
        greet(m, ((z + s) % 8) * 4 + q)
    for s in range(8):
        for other in range(2):
            if s or other:
                greet((m + s) % 8, z * 4 + ((yh + other) % 2) * 2 + c)
    greet(m, z * 4 + yh * 2 + (1 - c))
    greet(z, ((m + 7) % 8) * 4 + 3)
    greet(z, ((m + 1) % 8) * 4)

    @pl.when(rim_end)
    def _():
        for p in range(4):
            greet(rim_member, m * 4 + p)

    start = pl.multiple_of(m * PAIRS, 8)
    part = trans_ref[pl.ds(start, PAIRS), :].astype(BF16)
    raw = fac_ref[...]
    shares = raw / jnp.sum(raw, axis=0, keepdims=True)
    head = jnp.concatenate(
        [pts_ref[...].astype(F32), shares, jnp.zeros((HEAD - 6, BLOCK), F32)], axis=0
    ).astype(BF16)
    for j in range(4):
        zsend[j, 0:HEAD, :] = head[:, j * 128 : (j + 1) * 128]
        zsend[j, HEAD : HEAD + PAIRS, :] = part
        zsend[j, HEAD + PAIRS : PACKET, :] = jnp.zeros((8, POINTS), BF16)
    lane = lax.broadcasted_iota(jnp.int32, (PAIRS, POINTS), 1)
    packed = jnp.zeros((PAIRS, POINTS), F32)
    base = jnp.where(low_end, POINTS - RIM, 0)
    for b in range(8):
        block = trans_ref[b * PAIRS : (b + 1) * PAIRS, :]
        block = pltpu.roll(block, (b * RIM - base + POINTS) % POINTS, axis=1)
        packed = jnp.where(lane // RIM == b, block, packed)
    rimsend[0:PAIRS, :] = packed.astype(BF16)
    rimsend[PAIRS:208, :] = jnp.zeros((8, POINTS), BF16)

    pl.semaphore_wait(barrier, jnp.where(rim_end, 29, 25))

    def copy(src, dst, send, recv, member, grid):
        return pltpu.make_async_remote_copy(
            src_ref=src, dst_ref=dst, send_sem=send, recv_sem=recv,
            device_id=(member, grid), device_id_type=MESH,
        )

    def z_copy(s):
        to = (z + s) % 8
        return copy(zsend.at[to // 2], zrecv.at[z], zs_send.at[s], zs_recv.at[z], m, to * 4 + q)

    def rim_copy(p):
        which = jnp.where(low_end, 0, 1)
        return copy(
            rimsend, rimbuf.at[which], rim_send.at[p], rim_recv.at[which], rim_member, m * 4 + p
        )

    for s in range(1, 8):
        z_copy(s).start()

    @pl.when(rim_end)
    def _():
        for p in range(4):
            rim_copy(p).start()

    zrecv[z] = zsend[z // 2]

    def state_copy(to):
        return copy(
            picked.at[to], gathered.at[m], st_send.at[to], st_recv.at[m], to, g
        )

    def pick(s, carry):
        to = (m + s + 1) % 8
        onehot_into(oh, hi_ref, ids_ref[pl.ds(to, 1), :])
        chosen = jnp.dot(prior_ref[...], oh[...], preferred_element_type=F32).astype(BF16)

        @pl.when(s < 7)
        def _():
            picked[to] = chosen
            state_copy(to).start()

        @pl.when(s == 7)
        def _():
            gathered[m] = chosen

        return carry

    lax.fori_loop(0, 8, pick, 0)

    for s in range(1, 8):
        frm = (z + s) % 8
        copy(zsend.at[0], zrecv.at[frm], zs_send.at[s], zs_recv.at[frm], m, g).wait_recv()

    def plane_copy(s, other):
        to = (m + s) % 8
        side = (yh + other) % 2
        return copy(
            zrecv.at[to], tbuf.at[c, m, yh], t_send.at[s * 2 + other], t_recv.at[m * 2 + yh],
            to, z * 4 + side * 2 + c,
        )

    for s in range(8):
        for other in range(2):
            if s or other:
                plane_copy(s, other).start()
    tbuf[c, m, yh] = zrecv[m]

    for s in range(1, 8):
        frm = (m + s) % 8
        copy(picked.at[frm], gathered.at[frm], st_send.at[frm], st_recv.at[frm], frm, g).wait_recv()

    mean[...] = jnp.zeros((FIELDS, BLOCK), F32)

    def add_up(r, carry):
        part_sum = mean[...]
        for k in range(LOCAL):
            part_sum = part_sum + gathered[r, k * FIELDS : (k + 1) * FIELDS, :].astype(F32)
        mean[...] = part_sum
        return carry

    lax.fori_loop(0, GROUPS, add_up, 0)
    mean[...] = mean[...] / MEMBERS

    def deviate(r, carry):
        for k in range(LOCAL):
            x = gathered[r, k * FIELDS : (k + 1) * FIELDS, :].astype(F32)
            row = pl.multiple_of((r * LOCAL + k) * FIELDS, 8)
            dev[pl.ds(row, FIELDS), :] = (x - mean[...]).astype(BF16).astype(F32)
        return carry

    lax.fori_loop(0, GROUPS, deviate, 0)

    for s in range(8):
        for other in range(2):
            if s or other:
                frm, side = (m + s) % 8, (yh + other) % 2
                copy(
                    zrecv.at[frm], tbuf.at[c, frm, side], t_send.at[s * 2 + other],
                    t_recv.at[frm * 2 + side], frm, z * 4 + side * 2 + c,
                ).wait_recv()
    core_copy = copy(
        tbuf.at[c], tbuf.at[c], d_sems.at[0], d_sems.at[1], m, z * 4 + yh * 2 + (1 - c)
    )
    core_copy.start()
    copy(
        tbuf.at[1 - c], tbuf.at[1 - c], d_sems.at[0], d_sems.at[1], m, z * 4 + yh * 2 + (1 - c)
    ).wait_recv()
    copy(rimsend, rimbuf.at[0], rim_send.at[0], rim_recv.at[0], z, ((m + 7) % 8) * 4 + 3).wait_recv()
    copy(rimsend, rimbuf.at[1], rim_send.at[1], rim_recv.at[1], z, ((m + 1) % 8) * 4).wait_recv()

    offset = (z % 2) * 64 + q * 16
    lane16 = lax.broadcasted_iota(jnp.int32, (HEAD, POINTS), 1) // 16
    depth = lax.broadcasted_iota(jnp.int32, (BLOCK, POINTS), 0)
    params = []
    for p in range(4):
        gathered_head = jnp.zeros((HEAD, POINTS), F32)
        for r in range(8):
            tile = tbuf[p % 2, r, p // 2, 0:HEAD, :].astype(F32)
            tile = pltpu.roll(tile, (r * 16 - offset + POINTS) % POINTS, axis=1)
            gathered_head = jnp.where(lane16 == r, tile, gathered_head)
        params.append(gathered_head)
        column = jnp.zeros((BLOCK, POINTS), F32)
        for w in range(3):
            point = gathered_head[w : w + 1, :].astype(jnp.int32) + (p * POINTS - RIM)
            column = column + jnp.where(depth == point, gathered_head[w + 3 : w + 4, :], 0.0)
        spread[:, p * POINTS : (p + 1) * POINTS] = column.astype(BF16)

    rim_depth = lax.broadcasted_iota(jnp.int32, (POINTS, POINTS), 0)

    def blend(r, carry):
        shifted = rim_depth - r * RIM
        inside = rim_depth // RIM == r
        for end, p, back in ((0, 0, 0), (1, 3, POINTS + RIM)):
            column = jnp.zeros((POINTS, POINTS), F32)
            for w in range(3):
                point = params[p][w : w + 1, :].astype(jnp.int32) - back
                hit = jnp.logical_and(inside, shifted == point)
                column = column + jnp.where(hit, params[p][w + 3 : w + 4, :], 0.0)
            spread_rim[end] = column.astype(BF16)
        rows = jnp.concatenate(
            [tbuf[p % 2, r, p // 2, HEAD : HEAD + PAIRS, :] for p in range(4)], axis=1
        )
        main = jnp.dot(rows, spread[...], preferred_element_type=F32)
        lo = jnp.dot(rimbuf[0, 0:PAIRS, :], spread_rim[0], preferred_element_type=F32)
        hi = jnp.dot(rimbuf[1, 0:PAIRS, :], spread_rim[1], preferred_element_type=F32)
        whole = jnp.concatenate(
            [main[:, 0:128] + lo, main[:, 128:384], main[:, 384:512] + hi], axis=1
        )
        whole = whole.astype(BF16).astype(F32)
        for k in range(LOCAL):
            for to in range(GROUPS):
                row = k * MEMBERS + to * LOCAL
                weights[r * LOCAL + k, to, 0:LOCAL, :] = whole[row : row + LOCAL, :]
        return carry

    lax.fori_loop(0, GROUPS, blend, 0)

    def return_copy(to):
        return copy(result.at[to], returned.at[m], rt_send.at[to], rt_recv.at[m], to, g)

    def analyse(s, carry):
        to = (m + s + 1) % 8
        for b in range(4):
            lanes = slice(b * 128, (b + 1) * 128)

            def step(k, sums):
                x = dev[pl.ds(pl.multiple_of(k * FIELDS, 8), FIELDS), lanes]
                return tuple(
                    sums[j] + x * weights[k, to, j : j + 1, lanes] for j in range(LOCAL)
                )

            sums = lax.fori_loop(
                0, MEMBERS, step, tuple(jnp.zeros((FIELDS, 128), F32) for _ in range(LOCAL))
            )
            for j in range(LOCAL):
                value = (sums[j] + mean[:, lanes]).astype(BF16)

                @pl.when(s < 7)
                def _():
                    result[to, j * FIELDS : (j + 1) * FIELDS, lanes] = value

                @pl.when(s == 7)
                def _():
                    returned[m, j * FIELDS : (j + 1) * FIELDS, lanes] = value

        @pl.when(s < 7)
        def _():
            return_copy(to).start()

        return carry

    lax.fori_loop(0, 8, analyse, 0)

    total[...] = jnp.zeros((ROWS, PATCH), F32)

    def place(s, carry):
        frm = (m + 8 - s) % 8

        @pl.when(s > 0)
        def _():
            copy(
                result.at[frm], returned.at[frm], rt_send.at[frm], rt_recv.at[frm], frm, g
            ).wait_recv()

        onehot_into(oh, hi_ref, ids_ref[pl.ds(frm, 1), :])
        for b in range(8):
            cells = slice(b * 512, (b + 1) * 512)
            total[:, cells] += lax.dot_general(
                returned[frm], oh[cells, :], (((1,), (1,)), ((), ())), preferred_element_type=F32
            )
        return carry

    lax.fori_loop(0, 8, place, 0)
    out_ref[...] = total[...].astype(BF16)

    for s in range(1, 8):
        z_copy(s).wait_send()
        state_copy((m + s) % 8).wait_send()
        return_copy((m + s) % 8).wait_send()
    for s in range(8):
        for other in range(2):
            if s or other:
                plane_copy(s, other).wait_send()
    core_copy.wait_send()

    @pl.when(rim_end)
    def _():
        for p in range(4):
            rim_copy(p).wait_send()


def on_device(prior, mapping, triples, factors, transforms):
    ids = mapping.reshape(GROUPS, BLOCK)
    vmem = pl.BlockSpec(memory_space=pltpu.VMEM)
    dma = pltpu.SemaphoreType.DMA
    out = pl.pallas_call(
        kernel,
        out_shape=jax.ShapeDtypeStruct((ROWS, PATCH), BF16),
        in_specs=[vmem] * 5,
        out_specs=vmem,
        scratch_shapes=[
            pltpu.VMEM((4, PACKET, POINTS), BF16),
            pltpu.VMEM((8, PACKET, POINTS), BF16),
            pltpu.VMEM((2, 8, 2, PACKET, POINTS), BF16),
            pltpu.VMEM((208, POINTS), BF16),
            pltpu.VMEM((2, 208, POINTS), BF16),
            pltpu.VMEM((8, ROWS, BLOCK), BF16),
            pltpu.VMEM((8, ROWS, BLOCK), BF16),
            pltpu.VMEM((FIELDS, BLOCK), F32),
            pltpu.VMEM((MEMBERS * FIELDS, BLOCK), F32),
            pltpu.VMEM((MEMBERS, GROUPS, 8, BLOCK), F32),
            pltpu.VMEM((8, ROWS, BLOCK), BF16),
            pltpu.VMEM((8, ROWS, BLOCK), BF16),
            pltpu.VMEM((ROWS, PATCH), F32),
            pltpu.VMEM((PATCH, BLOCK), BF16),
            pltpu.VMEM((64, BLOCK), F32),
            pltpu.VMEM((BLOCK, BLOCK), BF16),
            pltpu.VMEM((2, POINTS, POINTS), BF16),
            dma((8,)), dma((8,)), dma((16,)), dma((16,)), dma((2,)), dma((4,)), dma((2,)),
            dma((8,)), dma((8,)), dma((8,)), dma((8,)),
        ],
        compiler_params=pltpu.CompilerParams(
            collective_id=0, has_side_effects=True, vmem_limit_bytes=62 * 1024 * 1024
        ),
    )(prior.reshape(ROWS, PATCH), ids, triples[0], factors[0], transforms)
    return out.reshape(LOCAL, FIELDS, PATCH)


def solution(mesh):
    return jax.shard_map(
        on_device,
        mesh=mesh,
        in_specs=(
            P("member", None, "grid"),
            P(None, None, "grid"),
            P("grid", None, "member"),
            P("grid", None, "member"),
            P(None, "grid"),
        ),
        out_specs=P("member", None, "grid"),
        check_vma=False,
    )
```

```python
import functools

import jax
import jax.numpy as jnp
from jax import lax
from jax.experimental import pallas as pl
from jax.experimental.pallas import tpu as pltpu
from jax.sharding import PartitionSpec as P

MESH = pl.DeviceIdType.MESH
F32, BF16 = jnp.float32, jnp.bfloat16

MEMBERS = 40
LOCAL = 5
FIELDS = 48
ROWS = LOCAL * FIELDS
PATCH = 4096
BLOCK = 512
GROUPS = 8
POINTS = 128
RIM = 16
PAIRS = 200
HEAD = 16


def onehot_into(oh_ref, hi_ref, ids):
    hi, lo = ids >> 6, ids & 63
    level = lax.broadcasted_iota(jnp.int32, (64, BLOCK), 0)
    hi_ref[...] = jnp.where(level == hi, 1.0, 0.0).astype(F32)
    low = jnp.where(level == lo, 1.0, 0.0).astype(BF16).reshape(4, 16, BLOCK)
    for h in range(64):
        row = jnp.broadcast_to(hi_ref[h : h + 1, :], (16, BLOCK)).astype(BF16)
        oh_ref[h * 64 : (h + 1) * 64, :] = (low * row[None]).reshape(64, BLOCK)


def kernel(
    prior_ref, map_ref, pts_ref, fac_ref, trans_ref, out_ref,
    ids_ref, zsend, zrecv, pbuf, tsend, tbuf, rimsend, rimbuf, picked, gathered, mean, dev,
    weights, result, returned, total, oh, hi_ref, params, spread, spread_rim,
    zs_send, zs_recv, p_send, p_recv, d_sems, rim_send, rim_recv, y_send, t_send, t_back,
    t_recv, c_send, c_recv, st_send, st_recv, rt_send, rt_recv,
):
    m, g = lax.axis_index("member"), lax.axis_index("grid")
    z, q = g // 4, g % 4
    yh, c = q // 2, q % 2
    rim_end = jnp.logical_or(q == 0, q == 3)
    low_end = q == 3
    rim_member = jnp.where(low_end, (z + 1) % 8, (z + 7) % 8)
    far = (z - m + 8) % 8
    root, tail = far == 0, far == 4
    passes_on = jnp.logical_and(far != 4, far != 5)
    ahead = jnp.where(far <= 3, (z + 1) % 8, (z + 7) % 8)
    near = jnp.logical_or(far == 1, far == 7)

    barrier = pltpu.get_barrier_semaphore()

    def greet(member, grid):
        pl.semaphore_signal(barrier, inc=1, device_id=(member, grid), device_id_type=MESH)

    for s in range(1, 8):
        greet(m, ((z + s) % 8) * 4 + q)
    for s in range(8):
        for other in range(2):
            if s or other:
                greet((m + s) % 8, z * 4 + ((yh + other) % 2) * 2 + c)
    greet(m, z * 4 + yh * 2 + (1 - c))
    greet(z, ((m + 7) % 8) * 4 + 3)
    greet(z, ((m + 1) % 8) * 4)

    @pl.when(rim_end)
    def _():
        for p in range(4):
            greet(rim_member, m * 4 + p)

    mapping = map_ref[...].reshape(GROUPS * 16, 32)
    mapping = jnp.concatenate([mapping, jnp.zeros((GROUPS * 16, 96), jnp.int32)], axis=1)
    mapping = jnp.transpose(mapping)
    for to in range(GROUPS):
        ids_ref[to] = mapping[to * 4 : (to + 1) * 4, :]

    def ids_of(to):
        return jnp.concatenate([ids_ref[to, p : p + 1, :] for p in range(4)], axis=1)

    raw = [fac_ref[w] for w in range(3)]
    raw_sum = raw[0] + raw[1] + raw[2]
    head = jnp.concatenate(
        [pts_ref[w].astype(F32) for w in range(3)]
        + [raw[w] / raw_sum for w in range(3)]
        + [jnp.zeros((HEAD - 6, BLOCK), F32)],
        axis=0,
    ).astype(BF16)
    for j in range(4):
        zsend[j] = head[:, j * 128 : (j + 1) * 128]
    lane = lax.broadcasted_iota(jnp.int32, (PAIRS, POINTS), 1)
    packed = jnp.zeros((PAIRS, POINTS), F32)
    base = jnp.where(low_end, POINTS - RIM, 0)
    for b in range(8):
        block = trans_ref[b * PAIRS : (b + 1) * PAIRS, :]
        tsend[b] = block.astype(BF16)

        @pl.when(root)
        def _():
            tbuf[c, b, yh] = trans_ref[b * PAIRS : (b + 1) * PAIRS, :].astype(BF16)

        block = pltpu.roll(block, (b * RIM - base + POINTS) % POINTS, axis=1)
        packed = jnp.where(lane // RIM == b, block, packed)
    rimsend[...] = packed.astype(BF16)

    pl.semaphore_wait(barrier, jnp.where(rim_end, 29, 25))

    def copy(src, dst, send, recv, member, grid):
        return pltpu.make_async_remote_copy(
            src_ref=src, dst_ref=dst, send_sem=send, recv_sem=recv,
            device_id=(member, grid), device_id_type=MESH,
        )

    def z_copy(s):
        to = (z + s) % 8
        return copy(zsend.at[to // 2], zrecv.at[z], zs_send.at[s], zs_recv.at[z], m, to * 4 + q)

    def rim_copy(p):
        which = jnp.where(low_end, 0, 1)
        return copy(
            rimsend, rimbuf.at[which], rim_send.at[p], rim_recv.at[which], rim_member, m * 4 + p
        )

    def y_copy(r):
        return copy(
            tsend.at[r], tbuf.at[c, r, yh], y_send.at[r], t_recv.at[yh * 8 + r],
            (m + 4) % 8, z * 4 + (1 - yh) * 2 + c,
        )

    def t_copy(r, side, sems, to):
        slot = side * 8 + r
        return copy(
            tbuf.at[c, r, side], tbuf.at[c, r, side], sems.at[slot], t_recv.at[slot],
            m, to * 4 + q,
        )

    def c_copy(core, r, side):
        slot = side * 8 + r
        return copy(
            tbuf.at[core, r, side], tbuf.at[core, r, side], c_send.at[slot], c_recv.at[slot],
            m, z * 4 + yh * 2 + (1 - c),
        )

    for s in range(1, 8):
        z_copy(s).start()

    @pl.when(tail)
    def _():
        for r in range(8):
            y_copy(r).start()

    @pl.when(rim_end)
    def _():
        for p in range(4):
            rim_copy(p).start()

    zrecv[z] = zsend[z // 2]

    def relay(r):
        for other in range(2):
            side = (yh + other) % 2
            if other:
                t_copy(r, side, t_send, ahead).wait_recv()
            else:

                @pl.when(jnp.logical_not(root))
                def _():
                    t_copy(r, side, t_send, ahead).wait_recv()

            @pl.when(passes_on)
            def _():
                t_copy(r, side, t_send, ahead).start()

            @pl.when(root)
            def _():
                t_copy(r, side, t_back, (z + 7) % 8).start()

            c_copy(c, r, side).start()

    def turn(s, sign):
        dx = jnp.where(
            jnp.logical_or(s == 0, s == 4), 1,
            jnp.where(
                jnp.logical_or(s == 2, s == 5), 3,
                jnp.where(jnp.logical_or(s == 3, s == 6), 2, 0),
            ),
        )
        dy = jnp.where(jnp.logical_or(s == 1, jnp.logical_and(s >= 4, s <= 6)), 1, 0)
        return ((m // 4 + dy) % 2) * 4 + (m % 4 + 4 + sign * dx) % 4

    def state_copy(to):
        return copy(picked.at[to], gathered.at[m], st_send.at[to], st_recv.at[m], to, g)

    def return_copy(to):
        return copy(result.at[to], returned.at[m], rt_send.at[to], rt_recv.at[m], to, g)

    def start_pieces(src, dst, send, recv, turns):
        for k in range(LOCAL):
            for t in turns:
                to = turn(t, 1)
                rows = pl.ds(k * FIELDS, FIELDS)
                copy(src.at[to, rows], dst.at[m, rows], send.at[to], recv.at[m], to, g).start()

    def param_copy(s, other):
        to = (m + s) % 8
        side = (yh + other) % 2
        return copy(
            zrecv.at[to], pbuf.at[c, m, yh], p_send.at[s * 2 + other], p_recv.at[m * 2 + yh],
            to, z * 4 + side * 2 + c,
        )

    def pick(s, carry):
        to = turn(s, 1)
        onehot_into(oh, hi_ref, ids_of(to))
        chosen = jnp.dot(prior_ref[...], oh[...], preferred_element_type=F32).astype(BF16)

        @pl.when(s < 7)
        def _():
            picked[to] = chosen

        @pl.when(s < 3)
        def _():
            state_copy(to).start()

        @pl.when(s == 6)
        def _():
            start_pieces(picked, gathered, st_send, st_recv, (3, 4, 5, 6))

        @pl.when(s == 7)
        def _():
            gathered[m] = chosen

        @pl.when(s == 2)
        def _():
            for t in range(1, 8):
                frm = (z + t) % 8
                copy(zsend.at[0], zrecv.at[frm], zs_send.at[t], zs_recv.at[frm], m, g).wait_recv()
            for t in range(8):
                for other in range(2):
                    if t or other:
                        param_copy(t, other).start()
            pbuf[c, m, yh] = zrecv[m]

        ready = jnp.logical_or(
            jnp.logical_and(root, s >= 2),
            jnp.logical_and(near, jnp.logical_or(s == 5, s == 7)),
        )

        @pl.when(ready)
        def _():
            relay(jnp.where(root, s - 2, (s - 5) // 2))

        return carry

    lax.fori_loop(0, 8, pick, 0)
    relayed = jnp.where(root, 6, jnp.where(near, 2, 0))

    for s in range(8):
        for other in range(2):
            if s or other:
                frm, side = (m + s) % 8, (yh + other) % 2
                copy(
                    zrecv.at[frm], pbuf.at[c, frm, side], p_send.at[s * 2 + other],
                    p_recv.at[frm * 2 + side], frm, z * 4 + side * 2 + c,
                ).wait_recv()
    core_copy = copy(
        pbuf.at[c], pbuf.at[c], d_sems.at[0], d_sems.at[1], m, z * 4 + yh * 2 + (1 - c)
    )
    core_copy.start()

    mean[...] = jnp.zeros((FIELDS, BLOCK), F32)

    def add_up(s):
        frm = turn(s, -1)

        @pl.when(s < 7)
        def _():
            copy(
                picked.at[frm], gathered.at[frm], st_send.at[frm], st_recv.at[frm], frm, g
            ).wait_recv()

        part_sum = mean[...]
        for k in range(LOCAL):
            part_sum = part_sum + gathered[frm, k * FIELDS : (k + 1) * FIELDS, :].astype(F32)
        mean[...] = part_sum

    def prepare():
        copy(
            pbuf.at[1 - c], pbuf.at[1 - c], d_sems.at[0], d_sems.at[1], m, z * 4 + yh * 2 + (1 - c)
        ).wait_recv()
        copy(
            rimsend, rimbuf.at[0], rim_send.at[0], rim_recv.at[0], z, ((m + 7) % 8) * 4 + 3
        ).wait_recv()
        copy(
            rimsend, rimbuf.at[1], rim_send.at[1], rim_recv.at[1], z, ((m + 1) % 8) * 4
        ).wait_recv()
        offset = (z % 2) * 64 + q * 16
        lane16 = lax.broadcasted_iota(jnp.int32, (HEAD, POINTS), 1) // 16
        depth = lax.broadcasted_iota(jnp.int32, (BLOCK, POINTS), 0)
        for p in range(4):
            in_order = jnp.zeros((HEAD, POINTS), F32)
            for r in range(8):
                tile = pbuf[p % 2, r, p // 2].astype(F32)
                tile = pltpu.roll(tile, (r * 16 - offset + POINTS) % POINTS, axis=1)
                in_order = jnp.where(lane16 == r, tile, in_order)
            params[p] = in_order
            column = jnp.zeros((BLOCK, POINTS), F32)
            for w in range(3):
                point = in_order[w : w + 1, :].astype(jnp.int32) + (p * POINTS - RIM)
                column = column + jnp.where(depth == point, in_order[w + 3 : w + 4, :], 0.0)
            spread[:, p * POINTS : (p + 1) * POINTS] = column.astype(BF16)

    rim_depth = lax.broadcasted_iota(jnp.int32, (POINTS, POINTS), 0)

    def blend(r):
        for side in range(2):
            c_copy(1 - c, r, side).wait_recv()
        shifted = rim_depth - r * RIM
        inside = rim_depth // RIM == r
        for end, p, back in ((0, 0, 0), (1, 3, POINTS + RIM)):
            column = jnp.zeros((POINTS, POINTS), F32)
            for w in range(3):
                point = params[p, w : w + 1, :].astype(jnp.int32) - back
                hit = jnp.logical_and(inside, shifted == point)
                column = column + jnp.where(hit, params[p, w + 3 : w + 4, :], 0.0)
            spread_rim[end] = column.astype(BF16)
        rows = jnp.concatenate([tbuf[p % 2, r, p // 2] for p in range(4)], axis=1)
        main = jnp.dot(rows, spread[...], preferred_element_type=F32)
        lo = jnp.dot(rimbuf[0], spread_rim[0], preferred_element_type=F32)
        hi = jnp.dot(rimbuf[1], spread_rim[1], preferred_element_type=F32)
        whole = jnp.concatenate(
            [main[:, 0:128] + lo, main[:, 128:384], main[:, 384:512] + hi], axis=1
        )
        whole = whole.astype(BF16).astype(F32)
        for k in range(LOCAL):
            for to in range(GROUPS):
                row = k * MEMBERS + to * LOCAL
                weights[r * LOCAL + k, to, 0:LOCAL, :] = whole[row : row + LOCAL, :]

    def arrive(r, carry):
        @pl.when(jnp.logical_and(r >= relayed, r < 8))
        def _():
            relay(r)

        @pl.when(r == 1)
        def _():
            prepare()

        @pl.when(r < 4)
        def _():
            add_up((r + 7) % 8)

        @pl.when(r >= 1)
        def _():
            blend(r - 1)

        return carry

    lax.fori_loop(0, 9, arrive, 0)

    def add_rest(s, carry):
        add_up(s)
        return carry

    lax.fori_loop(3, 7, add_rest, 0)
    mean[...] = mean[...] / MEMBERS

    def deviate(r, carry):
        for k in range(LOCAL):
            x = gathered[r, k * FIELDS : (k + 1) * FIELDS, :].astype(F32)
            row = pl.multiple_of((r * LOCAL + k) * FIELDS, 8)
            dev[pl.ds(row, FIELDS), :] = (x - mean[...]).astype(BF16).astype(F32)
        return carry

    lax.fori_loop(0, GROUPS, deviate, 0)

    def analyse(s, carry):
        to = turn(s, 1)
        for b in range(4):
            lanes = slice(b * 128, (b + 1) * 128)

            def step(i, sums):
                sums = list(sums)
                for k in range(8):
                    row = pl.multiple_of((i * 8 + k) * FIELDS, 8)
                    x = dev[pl.ds(row, FIELDS), lanes]
                    for j in range(LOCAL):
                        sums[j] = sums[j] + x * weights[i * 8 + k, to, j : j + 1, lanes]
                return tuple(sums)

            sums = lax.fori_loop(
                0, MEMBERS // 8, step, tuple(jnp.zeros((FIELDS, 128), F32) for _ in range(LOCAL))
            )
            for j in range(LOCAL):
                value = (sums[j] + mean[:, lanes]).astype(BF16)

                @pl.when(s < 7)
                def _():
                    result[to, j * FIELDS : (j + 1) * FIELDS, lanes] = value

                @pl.when(s == 7)
                def _():
                    returned[m, j * FIELDS : (j + 1) * FIELDS, lanes] = value

        @pl.when(s < 3)
        def _():
            return_copy(to).start()

        @pl.when(s == 4)
        def _():
            start_pieces(result, returned, rt_send, rt_recv, (3, 4))

        @pl.when(s == 6)
        def _():
            start_pieces(result, returned, rt_send, rt_recv, (5, 6))

        return carry

    lax.fori_loop(0, 8, analyse, 0)

    total[...] = jnp.zeros((ROWS, PATCH), F32)

    def place(i, carry):
        s = (i + 7) % 8
        frm = turn(s, -1)

        @pl.when(s < 7)
        def _():
            copy(
                result.at[frm], returned.at[frm], rt_send.at[frm], rt_recv.at[frm], frm, g
            ).wait_recv()

        onehot_into(oh, hi_ref, ids_of(frm))
        for b in range(8):
            cells = slice(b * 512, (b + 1) * 512)
            total[:, cells] += lax.dot_general(
                returned[frm], oh[cells, :], (((1,), (1,)), ((), ())), preferred_element_type=F32
            )
        return carry

    lax.fori_loop(0, 8, place, 0)
    out_ref[...] = total[...].astype(BF16)

    for s in range(1, 8):
        z_copy(s).wait_send()
        state_copy((m + s) % 8).wait_send()
        return_copy((m + s) % 8).wait_send()
    for s in range(8):
        for other in range(2):
            if s or other:
                param_copy(s, other).wait_send()
    core_copy.wait_send()
    for r in range(8):
        for side in range(2):
            c_copy(c, r, side).wait_send()

            @pl.when(passes_on)
            def _():
                t_copy(r, side, t_send, ahead).wait_send()

            @pl.when(root)
            def _():
                t_copy(r, side, t_back, (z + 7) % 8).wait_send()

    @pl.when(tail)
    def _():
        for r in range(8):
            y_copy(r).wait_send()

    @pl.when(rim_end)
    def _():
        for p in range(4):
            rim_copy(p).wait_send()


def on_device(prior, mapping, triples, factors, transforms):
    mapping = jnp.transpose(mapping, (1, 2, 0))
    vmem = pl.BlockSpec(memory_space=pltpu.VMEM)
    dma = pltpu.SemaphoreType.DMA
    out = pl.pallas_call(
        kernel,
        out_shape=jax.ShapeDtypeStruct((ROWS, PATCH), BF16),
        in_specs=[vmem] * 5,
        out_specs=vmem,
        scratch_shapes=[
            pltpu.VMEM((GROUPS, 4, POINTS), jnp.int32),
            pltpu.VMEM((4, HEAD, POINTS), BF16),
            pltpu.VMEM((8, HEAD, POINTS), BF16),
            pltpu.VMEM((2, 8, 2, HEAD, POINTS), BF16),
            pltpu.VMEM((8, PAIRS, POINTS), BF16),
            pltpu.VMEM((2, 8, 2, PAIRS, POINTS), BF16),
            pltpu.VMEM((PAIRS, POINTS), BF16),
            pltpu.VMEM((2, PAIRS, POINTS), BF16),
            pltpu.VMEM((8, ROWS, BLOCK), BF16),
            pltpu.VMEM((8, ROWS, BLOCK), BF16),
            pltpu.VMEM((FIELDS, BLOCK), F32),
            pltpu.VMEM((MEMBERS * FIELDS, BLOCK), F32),
            pltpu.VMEM((MEMBERS, GROUPS, 8, BLOCK), F32),
            pltpu.VMEM((8, ROWS, BLOCK), BF16),
            pltpu.VMEM((8, ROWS, BLOCK), BF16),
            pltpu.VMEM((ROWS, PATCH), F32),
            pltpu.VMEM((PATCH, BLOCK), BF16),
            pltpu.VMEM((64, BLOCK), F32),
            pltpu.VMEM((4, HEAD, POINTS), F32),
            pltpu.VMEM((BLOCK, BLOCK), BF16),
            pltpu.VMEM((2, POINTS, POINTS), BF16),
            dma((8,)), dma((8,)), dma((16,)), dma((16,)), dma((2,)), dma((4,)), dma((2,)),
            dma((8,)), dma((16,)), dma((16,)), dma((16,)), dma((16,)), dma((16,)),
            dma((8,)), dma((8,)), dma((8,)), dma((8,)),
        ],
        compiler_params=pltpu.CompilerParams(
            collective_id=0, has_side_effects=True, vmem_limit_bytes=62 * 1024 * 1024
        ),
    )(
        prior.reshape(ROWS, PATCH), mapping, jnp.transpose(triples, (1, 0, 2)),
        jnp.transpose(factors, (1, 0, 2)), transforms,
    )
    return out.reshape(LOCAL, FIELDS, PATCH)


def solution(mesh):
    return jax.shard_map(
        on_device,
        mesh=mesh,
        in_specs=(
            P("member", None, "grid"),
            P(None, None, "grid"),
            P("grid", None, "member"),
            P("grid", None, "member"),
            P(None, "grid"),
        ),
        out_specs=P("member", None, "grid"),
        check_vma=False,
    )
```

```python
import functools

import jax
import jax.numpy as jnp
from jax import lax
from jax.experimental import pallas as pl
from jax.experimental.pallas import tpu as pltpu
from jax.sharding import PartitionSpec as P

MESH = pl.DeviceIdType.MESH
F32, BF16 = jnp.float32, jnp.bfloat16

MEMBERS = 40
LOCAL = 5
FIELDS = 48
ROWS = LOCAL * FIELDS
PATCH = 4096
BLOCK = 512
GROUPS = 8
POINTS = 128
RIM = 16
PAIRS = 200
LAG = 3
HEAD = 16


def onehot_into(oh_ref, hi_ref, ids):
    hi, lo = ids >> 6, ids & 63
    level = lax.broadcasted_iota(jnp.int32, (64, BLOCK), 0)
    hi_ref[...] = jnp.where(level == hi, 1.0, 0.0).astype(F32)
    low = jnp.where(level == lo, 1.0, 0.0).astype(BF16).reshape(4, 16, BLOCK)
    for h in range(64):
        row = jnp.broadcast_to(hi_ref[h : h + 1, :], (16, BLOCK)).astype(BF16)
        oh_ref[h * 64 : (h + 1) * 64, :] = (low * row[None]).reshape(64, BLOCK)


def kernel(
    prior_ref, map_ref, pts_ref, fac_ref, trans_ref, out_ref,
    ids_ref, zsend, zrecv, pbuf, tsend, tbuf, rimsend, rimbuf, picked, gathered, mean, dev,
    weights, result, returned, total, oh, hi_ref, params, spread, spread_rim,
    zs_send, zs_recv, p_send, p_recv, d_sems, rim_send, rim_recv, y_send, t_send, t_back,
    t_recv, c_send, c_recv, st_send, st_recv, rt_send, rt_recv,
):
    m, g = lax.axis_index("member"), lax.axis_index("grid")
    z, q = g // 4, g % 4
    yh, c = q // 2, q % 2
    half, plane = m // 4, m % 4
    native = yh == half
    far = [(z - plane + 8) % 8, (z - plane + 4) % 8]
    root = z % 4 == plane
    starts = [jnp.logical_and(far[b] == 0, native) for b in range(2)]
    passes_on = [jnp.logical_and(far[b] != 4, far[b] != 5) for b in range(2)]
    ahead = [jnp.where(far[b] <= 3, (z + 1) % 8, (z + 7) % 8) for b in range(2)]
    hops = [jnp.where(far[b] <= 4, far[b], 8 - far[b]) for b in range(2)]
    lag = [LAG * (hops[b] + jnp.where(native, 0, 1)) + 1 for b in range(2)]
    last = jnp.maximum(jnp.maximum(lag[0], lag[1]), 6) + 2
    pair = jnp.where(c == 1, z * 2 + yh + 1, z * 2 + yh + 15) % 16
    rim_member = (pair % 2) * 4 + (pair // 2) % 4
    rim_slot = (pair // 8) * 2 + 1 - c
    rim_plane = (m + 2) % 8
    rim_source = (z + 6) % 8

    def rim_from(p):
        mine = (plane + 4 * (p // 2)) * 2 + half
        other = (mine + 15) % 16 if p % 2 == 0 else (mine + 1) % 16
        return other * 2 + (1 - p % 2)

    barrier = pltpu.get_barrier_semaphore()

    def greet(member, grid):
        pl.semaphore_signal(barrier, inc=1, device_id=(member, grid), device_id_type=MESH)

    for s in range(1, 8):
        greet(m, ((z + s) % 8) * 4 + q)
    for s in range(8):
        for other in range(2):
            if s or other:
                greet((m + s) % 8, z * 4 + ((yh + other) % 2) * 2 + c)
    greet(m, z * 4 + yh * 2 + (1 - c))
    for p in range(4):
        greet(rim_member, rim_plane * 4 + p)
        greet(rim_source, rim_from(p))

    mapping = map_ref[...].reshape(GROUPS * 16, 32)
    mapping = jnp.concatenate([mapping, jnp.zeros((GROUPS * 16, 96), jnp.int32)], axis=1)
    mapping = jnp.transpose(mapping)
    for to in range(GROUPS):
        first = 4 * (to % 4) + 2 * (to // 4)
        ids_ref[to, 0:2, :] = mapping[first : first + 2, :]
        ids_ref[to, 2:4, :] = mapping[first + 16 : first + 18, :]

    def ids_of(to):
        return jnp.concatenate([ids_ref[to, p : p + 1, :] for p in range(4)], axis=1)

    raw = [fac_ref[w] for w in range(3)]
    raw_sum = raw[0] + raw[1] + raw[2]
    head = jnp.concatenate(
        [pts_ref[w].astype(F32) for w in range(3)]
        + [raw[w] / raw_sum for w in range(3)]
        + [jnp.zeros((HEAD - 6, BLOCK), F32)],
        axis=0,
    ).astype(BF16)
    for j in range(4):
        zsend[j] = head[:, j * 128 : (j + 1) * 128]
    lane = lax.broadcasted_iota(jnp.int32, (PAIRS, POINTS), 1)
    packed = jnp.zeros((PAIRS, POINTS), F32)
    base = jnp.where(c == 1, POINTS - RIM, 0)
    for b in range(8):
        block = trans_ref[b * PAIRS : (b + 1) * PAIRS, :]
        tsend[b] = block.astype(BF16)

        for own in range(2):

            @pl.when(starts[own])
            def _():
                tbuf[c, b, own] = trans_ref[b * PAIRS : (b + 1) * PAIRS, :].astype(BF16)

        block = pltpu.roll(block, (b * RIM - base + POINTS) % POINTS, axis=1)
        packed = jnp.where(lane // RIM == b, block, packed)
    rimsend[...] = packed.astype(BF16)

    pl.semaphore_wait(barrier, 31)

    def copy(src, dst, send, recv, member, grid):
        return pltpu.make_async_remote_copy(
            src_ref=src, dst_ref=dst, send_sem=send, recv_sem=recv,
            device_id=(member, grid), device_id_type=MESH,
        )

    def z_copy(s):
        to = (z + s) % 8
        return copy(
            zsend.at[to // 2], zrecv.at[z % 4, z // 4], zs_send.at[s], zs_recv.at[z], m, to * 4 + q
        )

    def rim_copy(p):
        return copy(
            rimsend, rimbuf.at[rim_slot], rim_send.at[p], rim_recv.at[rim_slot],
            rim_member, rim_plane * 4 + p,
        )

    def y_copy(r):
        own = z // 4
        return copy(
            tsend.at[r], tbuf.at[c, r, own], y_send.at[r], t_recv.at[own * 8 + r],
            (m + 4) % 8, z * 4 + (1 - yh) * 2 + c,
        )

    def t_copy(r, side, sems, to):
        slot = side * 8 + r
        return copy(
            tbuf.at[c, r, side], tbuf.at[c, r, side], sems.at[slot], t_recv.at[slot],
            m, to * 4 + q,
        )

    def c_copy(core, r, side):
        slot = side * 8 + r
        return copy(
            tbuf.at[core, r, side], tbuf.at[core, r, side], c_send.at[slot], c_recv.at[slot],
            m, z * 4 + yh * 2 + (1 - c),
        )

    for s in range(1, 8):
        z_copy(s).start()

    @pl.when(jnp.logical_and(root, jnp.logical_not(native)))
    def _():
        for r in range(8):
            y_copy(r).start()

    for b in range(2):

        @pl.when(starts[b])
        def _():
            for r in range(8):
                t_copy(r, b, t_send, (z + 1) % 8).start()
                t_copy(r, b, t_back, (z + 7) % 8).start()
                c_copy(c, r, b).start()

    for p in range(4):
        rim_copy(p).start()

    zrecv[z % 4, z // 4] = zsend[z // 2]

    def tick(t):
        for b in range(2):
            r = t - lag[b]
            due = jnp.logical_and(r >= 0, r < 8)

            @pl.when(jnp.logical_and(due, jnp.logical_not(starts[b])))
            def _():
                t_copy(r, b, t_send, ahead[b]).wait_recv()

                @pl.when(passes_on[b])
                def _():
                    t_copy(r, b, t_send, ahead[b]).start()

                @pl.when(far[b] == 0)
                def _():
                    t_copy(r, b, t_back, (z + 7) % 8).start()

                c_copy(c, r, b).start()

    def turn(s, sign):
        dx = jnp.where(
            jnp.logical_or(s == 0, s == 4), 1,
            jnp.where(
                jnp.logical_or(s == 2, s == 5), 3,
                jnp.where(jnp.logical_or(s == 3, s == 6), 2, 0),
            ),
        )
        dy = jnp.where(jnp.logical_or(s == 1, jnp.logical_and(s >= 4, s <= 6)), 1, 0)
        return ((m // 4 + dy) % 2) * 4 + (m % 4 + 4 + sign * dx) % 4

    def state_copy(to):
        return copy(picked.at[to], gathered.at[m], st_send.at[to], st_recv.at[m], to, g)

    def return_copy(to):
        return copy(result.at[to], returned.at[m], rt_send.at[to], rt_recv.at[m], to, g)

    def start_pieces(src, dst, send, recv, turns):
        for k in range(LOCAL):
            for t in turns:
                to = turn(t, 1)
                rows = pl.ds(k * FIELDS, FIELDS)
                copy(src.at[to, rows], dst.at[m, rows], send.at[to], recv.at[m], to, g).start()

    def param_copy(s, other):
        to_plane, side = (plane + s) % 4, (yh + other) % 2
        return copy(
            zrecv.at[to_plane], pbuf.at[c, m], p_send.at[s * 2 + other], p_recv.at[m],
            yh * 4 + to_plane, z * 4 + side * 2 + c,
        )

    def param_sends(act):
        for t in range(4):
            for other in range(2):
                if t or other:
                    act(param_copy(t, other))

        @pl.when(jnp.logical_not(native))
        def _():
            act(param_copy(0, 0))

    def pick(s, carry):
        to = turn(s, 1)
        onehot_into(oh, hi_ref, ids_of(to))
        chosen = jnp.dot(prior_ref[...], oh[...], preferred_element_type=F32).astype(BF16)

        @pl.when(s < 7)
        def _():
            picked[to] = chosen

        @pl.when(s < 3)
        def _():
            state_copy(to).start()

        @pl.when(s == 6)
        def _():
            start_pieces(picked, gathered, st_send, st_recv, (3, 4, 5, 6))

        @pl.when(s == 7)
        def _():
            gathered[m] = chosen

        @pl.when(s == 2)
        def _():
            for t in range(1, 8):
                frm = (z + t) % 8
                copy(
                    zsend.at[0], zrecv.at[frm % 4, frm // 4], zs_send.at[t], zs_recv.at[frm], m, g
                ).wait_recv()
            param_sends(lambda sent: sent.start())

            @pl.when(native)
            def _():
                pbuf[c, m] = zrecv[plane]

        tick(s)
        return carry

    lax.fori_loop(0, 8, pick, 0)

    def param_wait(frm):
        copy(
            zrecv.at[0], pbuf.at[c, frm], p_send.at[0], p_recv.at[frm], frm, z * 4 + half * 2 + c
        ).wait_recv()

    for s in range(1, 8):
        param_wait((m + s) % 8)

    @pl.when(jnp.logical_not(native))
    def _():
        param_wait(m)

    core_copy = copy(
        pbuf.at[c], pbuf.at[c], d_sems.at[0], d_sems.at[1], m, z * 4 + yh * 2 + (1 - c)
    )
    core_copy.start()

    mean[...] = jnp.zeros((FIELDS, BLOCK), F32)

    def add_up(s):
        frm = turn(s, -1)

        @pl.when(s < 7)
        def _():
            copy(
                picked.at[frm], gathered.at[frm], st_send.at[frm], st_recv.at[frm], frm, g
            ).wait_recv()

        part_sum = mean[...]
        for k in range(LOCAL):
            part_sum = part_sum + gathered[frm, k * FIELDS : (k + 1) * FIELDS, :].astype(F32)
        mean[...] = part_sum

    def prepare():
        copy(
            pbuf.at[1 - c], pbuf.at[1 - c], d_sems.at[0], d_sems.at[1], m, z * 4 + yh * 2 + (1 - c)
        ).wait_recv()
        for p in range(4):
            copy(
                rimsend, rimbuf.at[p], rim_send.at[p], rim_recv.at[p], rim_source, rim_from(p)
            ).wait_recv()
        offset = (z % 2) * 64 + q * 16
        lane16 = lax.broadcasted_iota(jnp.int32, (HEAD, POINTS), 1) // 16
        depth = lax.broadcasted_iota(jnp.int32, (BLOCK, POINTS), 0)
        for p in range(4):
            in_order = jnp.zeros((HEAD, POINTS), F32)
            for r in range(8):
                tile = pbuf[p % 2, r, p // 2].astype(F32)
                tile = pltpu.roll(tile, (r * 16 - offset + POINTS) % POINTS, axis=1)
                in_order = jnp.where(lane16 == r, tile, in_order)
            params[p] = in_order
            column = jnp.zeros((BLOCK, POINTS), F32)
            for w in range(3):
                point = in_order[w : w + 1, :].astype(jnp.int32) + (p * POINTS - RIM)
                hit = jnp.logical_and(depth == point, depth // 256 == p // 2)
                column = column + jnp.where(hit, in_order[w + 3 : w + 4, :], 0.0)
            spread[:, p * POINTS : (p + 1) * POINTS] = column.astype(BF16)

    rim_depth = lax.broadcasted_iota(jnp.int32, (POINTS, POINTS), 0)

    def blend(r):
        for side in range(2):
            c_copy(1 - c, r, side).wait_recv()
        shifted = rim_depth - r * RIM
        inside = rim_depth // RIM == r
        for p in range(4):
            column = jnp.zeros((POINTS, POINTS), F32)
            for w in range(3):
                point = params[p, w : w + 1, :].astype(jnp.int32) - (p % 2) * (POINTS + RIM)
                hit = jnp.logical_and(inside, shifted == point)
                column = column + jnp.where(hit, params[p, w + 3 : w + 4, :], 0.0)
            spread_rim[p] = column.astype(BF16)
        rows = jnp.concatenate([tbuf[p % 2, r, p // 2] for p in range(4)], axis=1)
        whole = jnp.dot(rows, spread[...], preferred_element_type=F32)
        ends = [
            jnp.dot(rimbuf[p], spread_rim[p], preferred_element_type=F32) for p in range(4)
        ]
        whole = whole + jnp.concatenate(ends, axis=1)
        whole = whole.astype(BF16).astype(F32)
        for k in range(LOCAL):
            for to in range(GROUPS):
                row = k * MEMBERS + to * LOCAL
                weights[r * LOCAL + k, to, 0:LOCAL, :] = whole[row : row + LOCAL, :]

    def arrive(t, carry):
        tick(t)

        @pl.when(t == 8)
        def _():
            prepare()

        @pl.when(t < 12)
        def _():
            add_up((t + 7) % 8)

        r = t - last

        @pl.when(jnp.logical_and(r >= 0, r < 8))
        def _():
            blend(r)

        return carry

    lax.fori_loop(8, 8 + 5 * LAG + 3, arrive, 0)

    def add_rest(s, carry):
        add_up(s)
        return carry

    lax.fori_loop(3, 7, add_rest, 0)
    mean[...] = mean[...] / MEMBERS

    def deviate(r, carry):
        for k in range(LOCAL):
            x = gathered[r, k * FIELDS : (k + 1) * FIELDS, :].astype(F32)
            row = pl.multiple_of((r * LOCAL + k) * FIELDS, 8)
            dev[pl.ds(row, FIELDS), :] = (x - mean[...]).astype(BF16).astype(F32)
        return carry

    lax.fori_loop(0, GROUPS, deviate, 0)

    def analyse(s, carry):
        to = turn(s, 1)
        for b in range(4):
            lanes = slice(b * 128, (b + 1) * 128)

            def step(i, sums):
                sums = list(sums)
                for k in range(8):
                    row = pl.multiple_of((i * 8 + k) * FIELDS, 8)
                    x = dev[pl.ds(row, FIELDS), lanes]
                    for j in range(LOCAL):
                        sums[j] = sums[j] + x * weights[i * 8 + k, to, j : j + 1, lanes]
                return tuple(sums)

            sums = lax.fori_loop(
                0, MEMBERS // 8, step, tuple(jnp.zeros((FIELDS, 128), F32) for _ in range(LOCAL))
            )
            for j in range(LOCAL):
                value = (sums[j] + mean[:, lanes]).astype(BF16)

                @pl.when(s < 7)
                def _():
                    result[to, j * FIELDS : (j + 1) * FIELDS, lanes] = value

                @pl.when(s == 7)
                def _():
                    returned[m, j * FIELDS : (j + 1) * FIELDS, lanes] = value

        @pl.when(s < 3)
        def _():
            return_copy(to).start()

        @pl.when(s == 4)
        def _():
            start_pieces(result, returned, rt_send, rt_recv, (3, 4))

        @pl.when(s == 6)
        def _():
            start_pieces(result, returned, rt_send, rt_recv, (5, 6))

        return carry

    lax.fori_loop(0, 8, analyse, 0)

    total[...] = jnp.zeros((ROWS, PATCH), F32)

    def place(i, carry):
        s = (i + 7) % 8
        frm = turn(s, -1)

        @pl.when(s < 7)
        def _():
            copy(
                result.at[frm], returned.at[frm], rt_send.at[frm], rt_recv.at[frm], frm, g
            ).wait_recv()

        onehot_into(oh, hi_ref, ids_of(frm))
        for b in range(8):
            cells = slice(b * 512, (b + 1) * 512)
            total[:, cells] += lax.dot_general(
                returned[frm], oh[cells, :], (((1,), (1,)), ((), ())), preferred_element_type=F32
            )
        return carry

    lax.fori_loop(0, 8, place, 0)
    out_ref[...] = total[...].astype(BF16)

    for s in range(1, 8):
        z_copy(s).wait_send()
        state_copy((m + s) % 8).wait_send()
        return_copy((m + s) % 8).wait_send()
    param_sends(lambda sent: sent.wait_send())
    core_copy.wait_send()
    for r in range(8):
        for b in range(2):
            c_copy(c, r, b).wait_send()

            @pl.when(passes_on[b])
            def _():
                t_copy(r, b, t_send, ahead[b]).wait_send()

            @pl.when(far[b] == 0)
            def _():
                t_copy(r, b, t_back, (z + 7) % 8).wait_send()

    @pl.when(jnp.logical_and(root, jnp.logical_not(native)))
    def _():
        for r in range(8):
            y_copy(r).wait_send()

    for p in range(4):
        rim_copy(p).wait_send()


def on_device(prior, mapping, triples, factors, transforms):
    mapping = jnp.transpose(mapping, (1, 2, 0))
    vmem = pl.BlockSpec(memory_space=pltpu.VMEM)
    dma = pltpu.SemaphoreType.DMA
    out = pl.pallas_call(
        kernel,
        out_shape=jax.ShapeDtypeStruct((ROWS, PATCH), BF16),
        in_specs=[vmem] * 5,
        out_specs=vmem,
        scratch_shapes=[
            pltpu.VMEM((GROUPS, 4, POINTS), jnp.int32),
            pltpu.VMEM((4, HEAD, POINTS), BF16),
            pltpu.VMEM((4, 2, HEAD, POINTS), BF16),
            pltpu.VMEM((2, 8, 2, HEAD, POINTS), BF16),
            pltpu.VMEM((8, PAIRS, POINTS), BF16),
            pltpu.VMEM((2, 8, 2, PAIRS, POINTS), BF16),
            pltpu.VMEM((PAIRS, POINTS), BF16),
            pltpu.VMEM((4, PAIRS, POINTS), BF16),
            pltpu.VMEM((8, ROWS, BLOCK), BF16),
            pltpu.VMEM((8, ROWS, BLOCK), BF16),
            pltpu.VMEM((FIELDS, BLOCK), F32),
            pltpu.VMEM((MEMBERS * FIELDS, BLOCK), F32),
            pltpu.VMEM((MEMBERS, GROUPS, 8, BLOCK), F32),
            pltpu.VMEM((8, ROWS, BLOCK), BF16),
            pltpu.VMEM((8, ROWS, BLOCK), BF16),
            pltpu.VMEM((ROWS, PATCH), F32),
            pltpu.VMEM((PATCH, BLOCK), BF16),
            pltpu.VMEM((64, BLOCK), F32),
            pltpu.VMEM((4, HEAD, POINTS), F32),
            pltpu.VMEM((BLOCK, BLOCK), BF16),
            pltpu.VMEM((4, POINTS, POINTS), BF16),
            dma((8,)), dma((8,)), dma((8,)), dma((8,)), dma((2,)), dma((4,)), dma((4,)),
            dma((8,)), dma((16,)), dma((16,)), dma((16,)), dma((16,)), dma((16,)),
            dma((8,)), dma((8,)), dma((8,)), dma((8,)),
        ],
        compiler_params=pltpu.CompilerParams(
            collective_id=0, has_side_effects=True, vmem_limit_bytes=62 * 1024 * 1024
        ),
    )(
        prior.reshape(ROWS, PATCH), mapping, jnp.transpose(triples, (1, 0, 2)),
        jnp.transpose(factors, (1, 0, 2)), transforms,
    )
    return out.reshape(LOCAL, FIELDS, PATCH)


def solution(mesh):
    return jax.shard_map(
        on_device,
        mesh=mesh,
        in_specs=(
            P("member", None, "grid"),
            P(None, None, "grid"),
            P("grid", None, "member"),
            P("grid", None, "member"),
            P(None, "grid"),
        ),
        out_specs=P("member", None, "grid"),
        check_vma=False,
    )
```

```python
import functools

import jax
import jax.numpy as jnp
from jax import lax
from jax.experimental import pallas as pl
from jax.experimental.pallas import tpu as pltpu
from jax.sharding import PartitionSpec as P

MESH = pl.DeviceIdType.MESH
F32, BF16 = jnp.float32, jnp.bfloat16

MEMBERS = 40
LOCAL = 5
FIELDS = 48
ROWS = LOCAL * FIELDS
PATCH = 4096
BLOCK = 512
GROUPS = 8
POINTS = 128
RIM = 16
PAIRS = 200
LAG = 3
HEAD = 16


def onehot_into(oh_ref, hi_ref, ids):
    hi, lo = ids >> 6, ids & 63
    level = lax.broadcasted_iota(jnp.int32, (64, BLOCK), 0)
    hi_ref[...] = jnp.where(level == hi, 1.0, 0.0).astype(F32)
    low = jnp.where(level == lo, 1.0, 0.0).astype(BF16).reshape(4, 16, BLOCK)
    for h in range(64):
        row = jnp.broadcast_to(hi_ref[h : h + 1, :], (16, BLOCK)).astype(BF16)
        oh_ref[h * 64 : (h + 1) * 64, :] = (low * row[None]).reshape(64, BLOCK)


def kernel(
    prior_ref, map_ref, pts_ref, fac_ref, trans_ref, out_ref,
    ids_ref, zsend, zrecv, pbuf, tsend, tbuf, rimsend, picked, gathered, mean, dev,
    weights, result, returned, total, oh, hi_ref, params, spread, spread_rim,
    zs_send, zs_recv, p_send, p_recv, d_sems, rim_send, y_send, t_send, t_back,
    t_recv, c_send, c_recv, st_send, st_recv, rt_send, rt_recv,
):
    m, g = lax.axis_index("member"), lax.axis_index("grid")
    z, q = g // 4, g % 4
    yh, c = q // 2, q % 2
    half, plane = m // 4, m % 4
    native = yh == half
    far = [(z - plane + 8) % 8, (z - plane + 4) % 8]
    root = z % 4 == plane
    starts = [jnp.logical_and(far[b] == 0, native) for b in range(2)]
    passes_on = [jnp.logical_and(far[b] != 4, far[b] != 5) for b in range(2)]
    ahead = [jnp.where(far[b] <= 3, (z + 1) % 8, (z + 7) % 8) for b in range(2)]
    hops = [jnp.where(far[b] <= 4, far[b], 8 - far[b]) for b in range(2)]
    lag = [LAG * (hops[b] + jnp.where(native, 0, 1)) + 1 for b in range(2)]
    last = jnp.maximum(lag[0], lag[1]) + 6
    pair = jnp.where(c == 1, z * 2 + yh + 1, z * 2 + yh + 15) % 16
    rim_member = (pair % 2) * 4 + (pair // 2) % 4
    level = pair // 2 == z
    rim_across = rim_member == (m + 4) % 8
    rim_here = jnp.logical_and(rim_member == m, level)
    rim_along = jnp.logical_and(rim_member == m, jnp.logical_not(level))
    mine = z * 2 + half
    rim_pair = jnp.where(c == 0, mine + 1, mine + 15) % 16
    rim_in = jnp.logical_and(jnp.logical_and(root, native), rim_pair // 2 != z)
    rim_out = jnp.logical_and(rim_across, jnp.logical_not(level))

    barrier = pltpu.get_barrier_semaphore()

    def greet(member, grid):
        pl.semaphore_signal(barrier, inc=1, device_id=(member, grid), device_id_type=MESH)

    for s in range(1, 8):
        greet(m, ((z + s) % 8) * 4 + q)
    for s in range(8):
        for other in range(2):
            if s or other:
                greet((m + s) % 8, z * 4 + ((yh + other) % 2) * 2 + c)
    greet(m, z * 4 + yh * 2 + (1 - c))

    @pl.when(rim_out)
    def _():
        greet((m + 4) % 8, pair * 2 + c)

    @pl.when(rim_in)
    def _():
        greet((m + 4) % 8, rim_pair * 2 + c)

    mapping = map_ref[...].reshape(GROUPS * 16, 32)
    mapping = jnp.concatenate([mapping, jnp.zeros((GROUPS * 16, 96), jnp.int32)], axis=1)
    mapping = jnp.transpose(mapping)
    for to in range(GROUPS):
        first = 4 * (to % 4) + 2 * (to // 4)
        ids_ref[to, 0:2, :] = mapping[first : first + 2, :]
        ids_ref[to, 2:4, :] = mapping[first + 16 : first + 18, :]

    def ids_of(to):
        return jnp.concatenate([ids_ref[to, p : p + 1, :] for p in range(4)], axis=1)

    raw = [fac_ref[w] for w in range(3)]
    raw_sum = raw[0] + raw[1] + raw[2]
    head = jnp.concatenate(
        [pts_ref[w].astype(F32) for w in range(3)]
        + [raw[w] / raw_sum for w in range(3)]
        + [jnp.zeros((HEAD - 6, BLOCK), F32)],
        axis=0,
    ).astype(BF16)
    for j in range(4):
        zsend[j] = head[:, j * 128 : (j + 1) * 128]
    lane = lax.broadcasted_iota(jnp.int32, (PAIRS, POINTS), 1)
    packed = jnp.zeros((PAIRS, POINTS), F32)
    base = jnp.where(c == 1, POINTS - RIM, 0)
    for b in range(8):
        block = trans_ref[b * PAIRS : (b + 1) * PAIRS, :]
        tsend[b] = block.astype(BF16)

        for own in range(2):

            @pl.when(starts[own])
            def _():
                tbuf[c, b, own] = trans_ref[b * PAIRS : (b + 1) * PAIRS, :].astype(BF16)

        block = pltpu.roll(block, (b * RIM - base + POINTS) % POINTS, axis=1)
        packed = jnp.where(lane // RIM == b, block, packed)
    rimsend[...] = packed.astype(BF16)

    pl.semaphore_wait(barrier, 23 + jnp.where(rim_out, 1, 0) + jnp.where(rim_in, 1, 0))

    def copy(src, dst, send, recv, member, grid):
        return pltpu.make_async_remote_copy(
            src_ref=src, dst_ref=dst, send_sem=send, recv_sem=recv,
            device_id=(member, grid), device_id_type=MESH,
        )

    def z_copy(s):
        to = (z + s) % 8
        return copy(
            zsend.at[to // 2], zrecv.at[z % 4, z // 4], zs_send.at[s], zs_recv.at[z], m, to * 4 + q
        )

    def rim_copy(member, grid):
        dst = pair // 8
        return copy(
            rimsend, tbuf.at[c, 8, dst], rim_send.at[0], t_recv.at[dst * 9 + 8], member, grid
        )

    across = rim_copy((m + 4) % 8, pair * 2 + c)
    along = rim_copy(m, (pair // 2) * 4 + yh * 2 + c)

    def y_copy(r):
        own = z // 4
        return copy(
            tsend.at[r], tbuf.at[c, r, own], y_send.at[r], t_recv.at[own * 9 + r],
            (m + 4) % 8, z * 4 + (1 - yh) * 2 + c,
        )

    def t_copy(r, side, sems, to):
        slot = side * 9 + r
        return copy(
            tbuf.at[c, r, side], tbuf.at[c, r, side], sems.at[slot], t_recv.at[slot],
            m, to * 4 + q,
        )

    def c_copy(core, r, side):
        slot = side * 9 + r
        return copy(
            tbuf.at[core, r, side], tbuf.at[core, r, side], c_send.at[slot], c_recv.at[slot],
            m, z * 4 + yh * 2 + (1 - c),
        )

    for s in range(1, 8):
        z_copy(s).start()

    @pl.when(jnp.logical_and(root, jnp.logical_not(native)))
    def _():
        for r in range(8):
            y_copy(r).start()

    @pl.when(rim_across)
    def _():
        across.start()

    @pl.when(rim_along)
    def _():
        along.start()

    @pl.when(rim_here)
    def _():
        tbuf[c, 8, pair // 8] = rimsend[...]

    def spread_out(r, b):
        t_copy(r, b, t_send, (z + 1) % 8).start()
        t_copy(r, b, t_back, (z + 7) % 8).start()
        c_copy(c, r, b).start()

    for b in range(2):

        @pl.when(starts[b])
        def _():
            for r in range(4):
                spread_out(r, b)

    zrecv[z % 4, z // 4] = zsend[z // 2]

    def tick(t):
        for b in range(2):
            place_in = t - lag[b]
            due = jnp.logical_and(place_in >= 0, place_in < 9)
            r = jnp.where(place_in < 4, place_in, jnp.where(place_in == 4, 8, place_in - 1))

            @pl.when(jnp.logical_and(due, jnp.logical_not(starts[b])))
            def _():
                here = jnp.logical_and(jnp.logical_and(r == 8, rim_here), far[b] == 0)

                @pl.when(jnp.logical_not(here))
                def _():
                    t_copy(r, b, t_send, ahead[b]).wait_recv()

                @pl.when(passes_on[b])
                def _():
                    t_copy(r, b, t_send, ahead[b]).start()

                @pl.when(far[b] == 0)
                def _():
                    t_copy(r, b, t_back, (z + 7) % 8).start()

                c_copy(c, r, b).start()

            @pl.when(jnp.logical_and(t == 1, starts[b]))
            def _():
                t_copy(8, b, t_send, ahead[b]).wait_recv()
                spread_out(8, b)
                for r in range(4, 8):
                    spread_out(r, b)

    def turn(s, sign):
        dx = jnp.where(
            jnp.logical_or(s == 0, s == 4), 1,
            jnp.where(
                jnp.logical_or(s == 2, s == 5), 3,
                jnp.where(jnp.logical_or(s == 3, s == 6), 2, 0),
            ),
        )
        dy = jnp.where(jnp.logical_or(s == 1, jnp.logical_and(s >= 4, s <= 6)), 1, 0)
        return ((m // 4 + dy) % 2) * 4 + (m % 4 + 4 + sign * dx) % 4

    def state_copy(to):
        return copy(picked.at[to], gathered.at[m], st_send.at[to], st_recv.at[m], to, g)

    def return_copy(to):
        return copy(result.at[to], returned.at[m], rt_send.at[to], rt_recv.at[m], to, g)

    def start_pieces(src, dst, send, recv, turns):
        for k in range(LOCAL):
            for t in turns:
                to = turn(t, 1)
                rows = pl.ds(k * FIELDS, FIELDS)
                copy(src.at[to, rows], dst.at[m, rows], send.at[to], recv.at[m], to, g).start()

    def param_copy(s, other):
        to_plane, side = (plane + s) % 4, (yh + other) % 2
        return copy(
            zrecv.at[to_plane], pbuf.at[c, m], p_send.at[s * 2 + other], p_recv.at[m],
            yh * 4 + to_plane, z * 4 + side * 2 + c,
        )

    def param_sends(act):
        for t in range(4):
            for other in range(2):
                if t or other:
                    act(param_copy(t, other))

        @pl.when(jnp.logical_not(native))
        def _():
            act(param_copy(0, 0))

    def pick(s, carry):
        to = turn(s, 1)
        onehot_into(oh, hi_ref, ids_of(to))
        chosen = jnp.dot(prior_ref[...], oh[...], preferred_element_type=F32).astype(BF16)

        @pl.when(s < 7)
        def _():
            picked[to] = chosen

        @pl.when(s < 3)
        def _():
            state_copy(to).start()

        @pl.when(s == 6)
        def _():
            start_pieces(picked, gathered, st_send, st_recv, (3, 4, 5, 6))

        @pl.when(s == 7)
        def _():
            gathered[m] = chosen

        @pl.when(s == 2)
        def _():
            for t in range(1, 8):
                frm = (z + t) % 8
                copy(
                    zsend.at[0], zrecv.at[frm % 4, frm // 4], zs_send.at[t], zs_recv.at[frm], m, g
                ).wait_recv()
            param_sends(lambda sent: sent.start())

            @pl.when(native)
            def _():
                pbuf[c, m] = zrecv[plane]

        tick(s)
        return carry

    lax.fori_loop(0, 8, pick, 0)

    def param_wait(frm):
        copy(
            zrecv.at[0], pbuf.at[c, frm], p_send.at[0], p_recv.at[frm], frm, z * 4 + half * 2 + c
        ).wait_recv()

    for s in range(1, 8):
        param_wait((m + s) % 8)

    @pl.when(jnp.logical_not(native))
    def _():
        param_wait(m)

    core_copy = copy(
        pbuf.at[c], pbuf.at[c], d_sems.at[0], d_sems.at[1], m, z * 4 + yh * 2 + (1 - c)
    )
    core_copy.start()

    mean[...] = jnp.zeros((FIELDS, BLOCK), F32)

    def add_up(s):
        frm = turn(s, -1)

        @pl.when(s < 7)
        def _():
            copy(
                picked.at[frm], gathered.at[frm], st_send.at[frm], st_recv.at[frm], frm, g
            ).wait_recv()

        part_sum = mean[...]
        for k in range(LOCAL):
            part_sum = part_sum + gathered[frm, k * FIELDS : (k + 1) * FIELDS, :].astype(F32)
        mean[...] = part_sum

    def prepare():
        copy(
            pbuf.at[1 - c], pbuf.at[1 - c], d_sems.at[0], d_sems.at[1], m, z * 4 + yh * 2 + (1 - c)
        ).wait_recv()
        offset = (z % 2) * 64 + q * 16
        lane16 = lax.broadcasted_iota(jnp.int32, (HEAD, POINTS), 1) // 16
        depth = lax.broadcasted_iota(jnp.int32, (BLOCK, POINTS), 0)
        for p in range(4):
            in_order = jnp.zeros((HEAD, POINTS), F32)
            for r in range(8):
                tile = pbuf[p % 2, r, p // 2].astype(F32)
                tile = pltpu.roll(tile, (r * 16 - offset + POINTS) % POINTS, axis=1)
                in_order = jnp.where(lane16 == r, tile, in_order)
            params[p] = in_order
            column = jnp.zeros((BLOCK, POINTS), F32)
            for w in range(3):
                point = in_order[w : w + 1, :].astype(jnp.int32) + (p * POINTS - RIM)
                hit = jnp.logical_and(depth == point, depth // 256 == p // 2)
                column = column + jnp.where(hit, in_order[w + 3 : w + 4, :], 0.0)
            spread[:, p * POINTS : (p + 1) * POINTS] = column.astype(BF16)

    rim_depth = lax.broadcasted_iota(jnp.int32, (POINTS, POINTS), 0)

    def blend(r, carry):
        for side in range(2):
            c_copy(1 - c, r, side).wait_recv()
        shifted = rim_depth - r * RIM
        inside = rim_depth // RIM == r
        for p in range(4):
            column = jnp.zeros((POINTS, POINTS), F32)
            for w in range(3):
                point = params[p, w : w + 1, :].astype(jnp.int32) - (p % 2) * (POINTS + RIM)
                hit = jnp.logical_and(inside, shifted == point)
                column = column + jnp.where(hit, params[p, w + 3 : w + 4, :], 0.0)
            spread_rim[p] = column.astype(BF16)
        rows = jnp.concatenate([tbuf[p % 2, r, p // 2] for p in range(4)], axis=1)
        whole = jnp.dot(rows, spread[...], preferred_element_type=F32)
        ends = [
            jnp.dot(tbuf[1 - p % 2, 8, p // 2], spread_rim[p], preferred_element_type=F32)
            for p in range(4)
        ]
        whole = whole + jnp.concatenate(ends, axis=1)
        whole = whole.astype(BF16).astype(F32)
        for k in range(LOCAL):
            for to in range(GROUPS):
                row = k * MEMBERS + to * LOCAL
                weights[r * LOCAL + k, to, 0:LOCAL, :] = whole[row : row + LOCAL, :]
        return carry

    def arrive(t, carry):
        tick(t)

        @pl.when(t == 8)
        def _():
            prepare()

        @pl.when(t < 12)
        def _():
            add_up((t + 7) % 8)

        j = t - last

        @pl.when(j == 0)
        def _():
            for side in range(2):
                c_copy(1 - c, 8, side).wait_recv()

        @pl.when(jnp.logical_and(j >= 0, j < 4))
        def _():
            lax.fori_loop(2 * j, 2 * j + 2, blend, 0)

        return carry

    lax.fori_loop(8, 5 * LAG + 11, arrive, 0)

    def add_rest(s, carry):
        add_up(s)
        return carry

    lax.fori_loop(3, 7, add_rest, 0)
    mean[...] = mean[...] / MEMBERS

    def deviate(r, carry):
        for k in range(LOCAL):
            x = gathered[r, k * FIELDS : (k + 1) * FIELDS, :].astype(F32)
            row = pl.multiple_of((r * LOCAL + k) * FIELDS, 8)
            dev[pl.ds(row, FIELDS), :] = (x - mean[...]).astype(BF16).astype(F32)
        return carry

    lax.fori_loop(0, GROUPS, deviate, 0)

    def analyse(s, carry):
        to = turn(s, 1)
        for b in range(4):
            lanes = slice(b * 128, (b + 1) * 128)

            def step(i, sums):
                sums = list(sums)
                for k in range(8):
                    row = pl.multiple_of((i * 8 + k) * FIELDS, 8)
                    x = dev[pl.ds(row, FIELDS), lanes]
                    for j in range(LOCAL):
                        sums[j] = sums[j] + x * weights[i * 8 + k, to, j : j + 1, lanes]
                return tuple(sums)

            sums = lax.fori_loop(
                0, MEMBERS // 8, step, tuple(jnp.zeros((FIELDS, 128), F32) for _ in range(LOCAL))
            )
            for j in range(LOCAL):
                value = (sums[j] + mean[:, lanes]).astype(BF16)

                @pl.when(s < 7)
                def _():
                    result[to, j * FIELDS : (j + 1) * FIELDS, lanes] = value

                @pl.when(s == 7)
                def _():
                    returned[m, j * FIELDS : (j + 1) * FIELDS, lanes] = value

        @pl.when(s < 3)
        def _():
            return_copy(to).start()

        @pl.when(s == 4)
        def _():
            start_pieces(result, returned, rt_send, rt_recv, (3, 4))

        @pl.when(s == 6)
        def _():
            start_pieces(result, returned, rt_send, rt_recv, (5, 6))

        return carry

    lax.fori_loop(0, 8, analyse, 0)

    total[...] = jnp.zeros((ROWS, PATCH), F32)

    def place(i, carry):
        s = (i + 7) % 8
        frm = turn(s, -1)

        @pl.when(s < 7)
        def _():
            copy(
                result.at[frm], returned.at[frm], rt_send.at[frm], rt_recv.at[frm], frm, g
            ).wait_recv()

        onehot_into(oh, hi_ref, ids_of(frm))
        for b in range(8):
            cells = slice(b * 512, (b + 1) * 512)
            total[:, cells] += lax.dot_general(
                returned[frm], oh[cells, :], (((1,), (1,)), ((), ())), preferred_element_type=F32
            )
        return carry

    lax.fori_loop(0, 8, place, 0)
    out_ref[...] = total[...].astype(BF16)

    for s in range(1, 8):
        z_copy(s).wait_send()
        state_copy((m + s) % 8).wait_send()
        return_copy((m + s) % 8).wait_send()
    param_sends(lambda sent: sent.wait_send())
    core_copy.wait_send()
    for r in range(9):
        for b in range(2):
            c_copy(c, r, b).wait_send()

            @pl.when(passes_on[b])
            def _():
                t_copy(r, b, t_send, ahead[b]).wait_send()

            @pl.when(far[b] == 0)
            def _():
                t_copy(r, b, t_back, (z + 7) % 8).wait_send()

    @pl.when(jnp.logical_and(root, jnp.logical_not(native)))
    def _():
        for r in range(8):
            y_copy(r).wait_send()

    @pl.when(rim_across)
    def _():
        across.wait_send()

    @pl.when(rim_along)
    def _():
        along.wait_send()


def on_device(prior, mapping, triples, factors, transforms):
    mapping = jnp.transpose(mapping, (1, 2, 0))
    vmem = pl.BlockSpec(memory_space=pltpu.VMEM)
    dma = pltpu.SemaphoreType.DMA
    out = pl.pallas_call(
        kernel,
        out_shape=jax.ShapeDtypeStruct((ROWS, PATCH), BF16),
        in_specs=[vmem] * 5,
        out_specs=vmem,
        scratch_shapes=[
            pltpu.VMEM((GROUPS, 4, POINTS), jnp.int32),
            pltpu.VMEM((4, HEAD, POINTS), BF16),
            pltpu.VMEM((4, 2, HEAD, POINTS), BF16),
            pltpu.VMEM((2, 8, 2, HEAD, POINTS), BF16),
            pltpu.VMEM((8, PAIRS, POINTS), BF16),
            pltpu.VMEM((2, 9, 2, PAIRS, POINTS), BF16),
            pltpu.VMEM((PAIRS, POINTS), BF16),
            pltpu.VMEM((8, ROWS, BLOCK), BF16),
            pltpu.VMEM((8, ROWS, BLOCK), BF16),
            pltpu.VMEM((FIELDS, BLOCK), F32),
            pltpu.VMEM((MEMBERS * FIELDS, BLOCK), F32),
            pltpu.VMEM((MEMBERS, GROUPS, 8, BLOCK), F32),
            pltpu.VMEM((8, ROWS, BLOCK), BF16),
            pltpu.VMEM((8, ROWS, BLOCK), BF16),
            pltpu.VMEM((ROWS, PATCH), F32),
            pltpu.VMEM((PATCH, BLOCK), BF16),
            pltpu.VMEM((64, BLOCK), F32),
            pltpu.VMEM((4, HEAD, POINTS), F32),
            pltpu.VMEM((BLOCK, BLOCK), BF16),
            pltpu.VMEM((4, POINTS, POINTS), BF16),
            dma((8,)), dma((8,)), dma((8,)), dma((8,)), dma((2,)), dma((1,)),
            dma((8,)), dma((18,)), dma((18,)), dma((18,)), dma((18,)), dma((18,)),
            dma((8,)), dma((8,)), dma((8,)), dma((8,)),
        ],
        compiler_params=pltpu.CompilerParams(
            collective_id=0, has_side_effects=True, vmem_limit_bytes=62 * 1024 * 1024
        ),
    )(
        prior.reshape(ROWS, PATCH), mapping, jnp.transpose(triples, (1, 0, 2)),
        jnp.transpose(factors, (1, 0, 2)), transforms,
    )
    return out.reshape(LOCAL, FIELDS, PATCH)


def solution(mesh):
    return jax.shard_map(
        on_device,
        mesh=mesh,
        in_specs=(
            P("member", None, "grid"),
            P(None, None, "grid"),
            P("grid", None, "member"),
            P("grid", None, "member"),
            P(None, "grid"),
        ),
        out_specs=P("member", None, "grid"),
        check_vma=False,
    )
```

```python
import functools

import jax
import jax.numpy as jnp
from jax import lax
from jax.experimental import pallas as pl
from jax.experimental.pallas import tpu as pltpu
from jax.sharding import PartitionSpec as P

MESH = pl.DeviceIdType.MESH
F32, BF16 = jnp.float32, jnp.bfloat16

MEMBERS = 40
LOCAL = 5
FIELDS = 48
ROWS = LOCAL * FIELDS
PATCH = 4096
BLOCK = 512
GROUPS = 8
POINTS = 128
RIM = 16
PAIRS = 200
LAG = 2
HEAD = 16


def onehot_into(oh_ref, hi_ref, ids):
    width = ids.shape[1]
    hi, lo = ids >> 6, ids & 63
    level = lax.broadcasted_iota(jnp.int32, (64, width), 0)
    hi_ref[:, 0:width] = jnp.where(level == hi, 1.0, 0.0).astype(F32)
    low = jnp.where(level == lo, 1.0, 0.0).astype(BF16).reshape(4, 16, width)
    for h in range(64):
        row = jnp.broadcast_to(hi_ref[h : h + 1, 0:width], (16, width)).astype(BF16)
        oh_ref[h * 64 : (h + 1) * 64, 0:width] = (low * row[None]).reshape(64, width)


def kernel(
    prior_ref, map_ref, pts_ref, fac_ref, trans_ref, out_ref,
    ids_ref, zsend, zrecv, pbuf, tsend, tbuf, rimsend, picked, gathered, mean, mean_of, dev,
    weights, result, returned, total, oh, hi_ref, params, spread, spread_rim,
    zs_send, zs_recv, p_send, p_recv, d_sems, rim_send, y_send, t_send, t_back,
    t_recv, c_send, c_recv, st_send, st_recv, rt_send, rt_recv,
):
    m, g = lax.axis_index("member"), lax.axis_index("grid")
    z, q = g // 4, g % 4
    yh, c = q // 2, q % 2
    half, plane = m // 4, m % 4
    native = yh == half
    far = [(z - plane + 8) % 8, (z - plane + 4) % 8]
    root = z % 4 == plane
    starts = [jnp.logical_and(far[b] == 0, native) for b in range(2)]
    passes_on = [jnp.logical_and(far[b] != 4, far[b] != 5) for b in range(2)]
    ahead = [jnp.where(far[b] <= 3, (z + 1) % 8, (z + 7) % 8) for b in range(2)]
    hops = [jnp.where(far[b] <= 4, far[b], 8 - far[b]) for b in range(2)]
    lag = [LAG * (hops[b] + jnp.where(native, 0, 1)) + 1 for b in range(2)]
    near = jnp.where(hops[0] <= hops[1], 0, 1)
    last = jnp.maximum(jnp.minimum(lag[0], lag[1]), 2) + 6
    turned = jnp.maximum(last + 4, 12)
    pair = jnp.where(c == 1, z * 2 + yh + 1, z * 2 + yh + 15) % 16
    rim_member = (pair % 2) * 4 + (pair // 2) % 4
    level = pair // 2 == z
    rim_across = rim_member == (m + 4) % 8
    rim_here = jnp.logical_and(rim_member == m, level)
    rim_along = jnp.logical_and(rim_member == m, jnp.logical_not(level))
    mine = z * 2 + half
    rim_pair = jnp.where(c == 0, mine + 1, mine + 15) % 16
    rim_in = jnp.logical_and(jnp.logical_and(root, native), rim_pair // 2 != z)
    rim_out = jnp.logical_and(rim_across, jnp.logical_not(level))

    barrier = pltpu.get_barrier_semaphore()

    def greet(member, grid):
        pl.semaphore_signal(barrier, inc=1, device_id=(member, grid), device_id_type=MESH)

    for s in range(1, 8):
        greet(m, ((z + s) % 8) * 4 + q)
    for s in range(8):
        for other in range(2):
            if s or other:
                greet((m + s) % 8, z * 4 + ((yh + other) % 2) * 2 + c)
    greet(m, z * 4 + yh * 2 + (1 - c))

    @pl.when(rim_out)
    def _():
        greet((m + 4) % 8, pair * 2 + c)

    @pl.when(rim_in)
    def _():
        greet((m + 4) % 8, rim_pair * 2 + c)

    mapping = map_ref[...].reshape(GROUPS * 16, 32)
    mapping = jnp.concatenate([mapping, jnp.zeros((GROUPS * 16, 96), jnp.int32)], axis=1)
    mapping = jnp.transpose(mapping)
    for to in range(GROUPS):
        first = 4 * (to % 4) + 2 * (to // 4)
        ids_ref[to, 0] = mapping[first : first + 2, :]
        ids_ref[to, 1] = mapping[first + 16 : first + 18, :]

    def half_ids(to, b):
        return jnp.concatenate([ids_ref[to, b, p : p + 1, :] for p in range(2)], axis=1)

    def ids_of(to):
        return jnp.concatenate([half_ids(to, b) for b in range(2)], axis=1)

    raw = [fac_ref[w] for w in range(3)]
    raw_sum = raw[0] + raw[1] + raw[2]
    head = jnp.concatenate(
        [pts_ref[w].astype(F32) for w in range(3)]
        + [raw[w] / raw_sum for w in range(3)]
        + [jnp.zeros((HEAD - 6, BLOCK), F32)],
        axis=0,
    ).astype(BF16)
    for j in range(4):
        zsend[j] = head[:, j * 128 : (j + 1) * 128]
    lane = lax.broadcasted_iota(jnp.int32, (PAIRS, POINTS), 1)
    packed = jnp.zeros((PAIRS, POINTS), F32)
    base = jnp.where(c == 1, POINTS - RIM, 0)
    for b in range(8):
        block = trans_ref[b * PAIRS : (b + 1) * PAIRS, :]
        tsend[b] = block.astype(BF16)

        for own in range(2):

            @pl.when(starts[own])
            def _():
                tbuf[c, b, own] = trans_ref[b * PAIRS : (b + 1) * PAIRS, :].astype(BF16)

        block = pltpu.roll(block, (b * RIM - base + POINTS) % POINTS, axis=1)
        packed = jnp.where(lane // RIM == b, block, packed)
    rimsend[...] = packed.astype(BF16)

    pl.semaphore_wait(barrier, 23 + jnp.where(rim_out, 1, 0) + jnp.where(rim_in, 1, 0))

    def copy(src, dst, send, recv, member, grid):
        return pltpu.make_async_remote_copy(
            src_ref=src, dst_ref=dst, send_sem=send, recv_sem=recv,
            device_id=(member, grid), device_id_type=MESH,
        )

    def z_copy(s):
        to = (z + s) % 8
        return copy(
            zsend.at[to // 2], zrecv.at[z % 4, z // 4], zs_send.at[s], zs_recv.at[z], m, to * 4 + q
        )

    def rim_copy(member, grid):
        dst = pair // 8
        return copy(
            rimsend, tbuf.at[c, 8, dst], rim_send.at[0], t_recv.at[dst * 9 + 8], member, grid
        )

    across = rim_copy((m + 4) % 8, pair * 2 + c)
    along = rim_copy(m, (pair // 2) * 4 + yh * 2 + c)

    def y_copy(r):
        own = z // 4
        return copy(
            tsend.at[r], tbuf.at[c, r, own], y_send.at[r], t_recv.at[own * 9 + r],
            (m + 4) % 8, z * 4 + (1 - yh) * 2 + c,
        )

    def t_copy(r, side, sems, to):
        slot = side * 9 + r
        return copy(
            tbuf.at[c, r, side], tbuf.at[c, r, side], sems.at[slot], t_recv.at[slot],
            m, to * 4 + q,
        )

    def c_copy(core, r, side):
        slot = side * 9 + r
        return copy(
            tbuf.at[core, r, side], tbuf.at[core, r, side], c_send.at[slot], c_recv.at[slot],
            m, z * 4 + yh * 2 + (1 - c),
        )

    for s in range(1, 8):
        z_copy(s).start()

    @pl.when(jnp.logical_and(root, jnp.logical_not(native)))
    def _():
        for r in range(8):
            y_copy(r).start()

    @pl.when(rim_across)
    def _():
        across.start()

    @pl.when(rim_along)
    def _():
        along.start()

    @pl.when(rim_here)
    def _():
        tbuf[c, 8, pair // 8] = rimsend[...]

    def spread_out(r, b):
        t_copy(r, b, t_send, (z + 1) % 8).start()
        t_copy(r, b, t_back, (z + 7) % 8).start()
        c_copy(c, r, b).start()

    for b in range(2):

        @pl.when(starts[b])
        def _():
            for r in range(4):
                spread_out(r, b)

    zrecv[z % 4, z // 4] = zsend[z // 2]

    def tick(t):
        for b in range(2):
            place_in = t - lag[b]
            due = jnp.logical_and(place_in >= 0, place_in < 9)
            r = jnp.where(place_in < 4, place_in, jnp.where(place_in == 4, 8, place_in - 1))

            @pl.when(jnp.logical_and(due, jnp.logical_not(starts[b])))
            def _():
                here = jnp.logical_and(jnp.logical_and(r == 8, rim_here), far[b] == 0)

                @pl.when(jnp.logical_not(here))
                def _():
                    t_copy(r, b, t_send, ahead[b]).wait_recv()

                @pl.when(passes_on[b])
                def _():
                    t_copy(r, b, t_send, ahead[b]).start()

                @pl.when(far[b] == 0)
                def _():
                    t_copy(r, b, t_back, (z + 7) % 8).start()

                c_copy(c, r, b).start()

            @pl.when(jnp.logical_and(t == 1, starts[b]))
            def _():
                t_copy(8, b, t_send, ahead[b]).wait_recv()
                spread_out(8, b)
                for r in range(4, 8):
                    spread_out(r, b)

    def turn(s, sign):
        dx = jnp.where(
            jnp.logical_or(s == 0, s == 4), 1,
            jnp.where(
                jnp.logical_or(s == 2, s == 5), 3,
                jnp.where(jnp.logical_or(s == 3, s == 6), 2, 0),
            ),
        )
        dy = jnp.where(jnp.logical_or(s == 1, jnp.logical_and(s >= 4, s <= 6)), 1, 0)
        return ((m // 4 + dy) % 2) * 4 + (m % 4 + 4 + sign * dx) % 4

    def state_copy(to):
        return copy(picked.at[to], gathered.at[m], st_send.at[to], st_recv.at[m], to, g)

    def return_copy(to, b):
        return copy(
            result.at[b, to], returned.at[b, m], rt_send.at[b * 8 + to], rt_recv.at[b * 8 + m],
            to, g,
        )

    def start_pieces(src, dst, send, recv, turns, shift=0):
        for k in range(LOCAL):
            for t in turns:
                to = turn(t, 1)
                rows = pl.ds(k * FIELDS, FIELDS)
                copy(
                    src.at[to, rows], dst.at[m, rows], send.at[shift + to], recv.at[shift + m],
                    to, g,
                ).start()

    def param_copy(s, other):
        to_plane, side = (plane + s) % 4, (yh + other) % 2
        return copy(
            zrecv.at[to_plane], pbuf.at[c, m], p_send.at[s * 2 + other], p_recv.at[m],
            yh * 4 + to_plane, z * 4 + side * 2 + c,
        )

    def param_sends(act):
        for t in range(4):
            for other in range(2):
                if t or other:
                    act(param_copy(t, other))

        @pl.when(jnp.logical_not(native))
        def _():
            act(param_copy(0, 0))

    def pick(s, carry):
        to = turn(s, 1)
        onehot_into(oh, hi_ref, ids_of(to))
        chosen = jnp.dot(prior_ref[...], oh[...], preferred_element_type=F32).astype(BF16)

        @pl.when(s < 7)
        def _():
            picked[to] = chosen

        @pl.when(s < 3)
        def _():
            state_copy(to).start()

        @pl.when(s == 6)
        def _():
            start_pieces(picked, gathered, st_send, st_recv, (3, 4, 5, 6))

        @pl.when(s == 7)
        def _():
            gathered[m] = chosen

        @pl.when(s == 2)
        def _():
            for t in range(1, 8):
                frm = (z + t) % 8
                copy(
                    zsend.at[0], zrecv.at[frm % 4, frm // 4], zs_send.at[t], zs_recv.at[frm], m, g
                ).wait_recv()
            param_sends(lambda sent: sent.start())

            @pl.when(native)
            def _():
                pbuf[c, m] = zrecv[plane]

        tick(s)
        return carry

    lax.fori_loop(0, 8, pick, 0)

    def param_wait(frm):
        copy(
            zrecv.at[0], pbuf.at[c, frm], p_send.at[0], p_recv.at[frm], frm, z * 4 + half * 2 + c
        ).wait_recv()

    for s in range(1, 8):
        param_wait((m + s) % 8)

    @pl.when(jnp.logical_not(native))
    def _():
        param_wait(m)

    core_copy = copy(
        pbuf.at[c], pbuf.at[c], d_sems.at[0], d_sems.at[1], m, z * 4 + yh * 2 + (1 - c)
    )
    core_copy.start()

    mean[...] = jnp.zeros((FIELDS, BLOCK), F32)

    def add_up(s):
        frm = turn(s, -1)

        @pl.when(s < 7)
        def _():
            copy(
                picked.at[frm], gathered.at[frm], st_send.at[frm], st_recv.at[frm], frm, g
            ).wait_recv()

        part_sum = mean[...]
        for k in range(LOCAL):
            part_sum = part_sum + gathered[frm, k * FIELDS : (k + 1) * FIELDS, :].astype(F32)
        mean[...] = part_sum

    def prepare():
        copy(
            pbuf.at[1 - c], pbuf.at[1 - c], d_sems.at[0], d_sems.at[1], m, z * 4 + yh * 2 + (1 - c)
        ).wait_recv()
        offset = (z % 2) * 64 + q * 16
        lane16 = lax.broadcasted_iota(jnp.int32, (HEAD, POINTS), 1) // 16
        depth = lax.broadcasted_iota(jnp.int32, (2 * POINTS, POINTS), 0)
        for p in range(4):
            in_order = jnp.zeros((HEAD, POINTS), F32)
            for r in range(8):
                tile = pbuf[p % 2, r, p // 2].astype(F32)
                tile = pltpu.roll(tile, (r * 16 - offset + POINTS) % POINTS, axis=1)
                in_order = jnp.where(lane16 == r, tile, in_order)
            params[p] = in_order
            column = jnp.zeros((2 * POINTS, POINTS), F32)
            for w in range(3):
                point = in_order[w : w + 1, :].astype(jnp.int32) + ((p % 2) * POINTS - RIM)
                column = column + jnp.where(depth == point, in_order[w + 3 : w + 4, :], 0.0)
            spread[p // 2, :, (p % 2) * POINTS : (p % 2 + 1) * POINTS] = column.astype(BF16)

    rim_depth = lax.broadcasted_iota(jnp.int32, (POINTS, POINTS), 0)

    def blend(r, b):
        c_copy(1 - c, r, b).wait_recv()
        shifted = rim_depth - r * RIM
        inside = rim_depth // RIM == r
        for p in range(2):
            column = jnp.zeros((POINTS, POINTS), F32)
            for w in range(3):
                point = params[2 * b + p, w : w + 1, :].astype(jnp.int32) - p * (POINTS + RIM)
                hit = jnp.logical_and(inside, shifted == point)
                column = column + jnp.where(hit, params[2 * b + p, w + 3 : w + 4, :], 0.0)
            spread_rim[p] = column.astype(BF16)
        rows = jnp.concatenate([tbuf[p, r, b] for p in range(2)], axis=1)
        whole = jnp.dot(rows, spread[b], preferred_element_type=F32)
        ends = [
            jnp.dot(tbuf[1 - p, 8, b], spread_rim[p], preferred_element_type=F32)
            for p in range(2)
        ]
        whole = whole + jnp.concatenate(ends, axis=1)
        whole = whole.astype(BF16).astype(F32)
        for k in range(LOCAL):
            for to in range(GROUPS):
                row = k * MEMBERS + to * LOCAL
                weights[b, r * LOCAL + k, to, 0:LOCAL, :] = whole[row : row + LOCAL, :]
        return b

    def arrive(t, carry):
        tick(t)

        @pl.when(t == 8)
        def _():
            prepare()

        @pl.when(t < 12)
        def _():
            add_up((t + 7) % 8)

        j = t - last

        @pl.when(j == 0)
        def _():
            c_copy(1 - c, 8, near).wait_recv()

        @pl.when(jnp.logical_and(j >= 0, j < 4))
        def _():
            lax.fori_loop(2 * j, 2 * j + 2, blend, near)

        return carry

    lax.fori_loop(8, turned, arrive, 0)

    def add_rest(s, carry):
        add_up(s)
        return carry

    lax.fori_loop(3, 7, add_rest, 0)
    for b in range(2):
        mean_of[b] = mean[:, b * 256 : (b + 1) * 256] / MEMBERS

    def deviate(r, carry):
        for k in range(LOCAL):
            row = pl.multiple_of((r * LOCAL + k) * FIELDS, 8)
            for b in range(2):
                x = gathered[r, k * FIELDS : (k + 1) * FIELDS, b * 256 : (b + 1) * 256]
                difference = x.astype(F32) - mean_of[b]
                dev[b, pl.ds(row, FIELDS), :] = difference.astype(BF16).astype(F32)
        return carry

    lax.fori_loop(0, GROUPS, deviate, 0)

    def analyse(i, carry):
        s, b = i % 8, jnp.where(i < 8, near, 1 - near)
        to = turn(s, 1)

        @pl.when(i < 8)
        def _():
            tick(turned + i)

        @pl.when(i == 8)
        def _():
            c_copy(1 - c, 8, b).wait_recv()
            lax.fori_loop(0, 8, blend, b)

        for half_lanes in range(2):
            lanes = slice(half_lanes * 128, (half_lanes + 1) * 128)

            def step(i, sums):
                sums = list(sums)
                for k in range(8):
                    row = pl.multiple_of((i * 8 + k) * FIELDS, 8)
                    x = dev[b, pl.ds(row, FIELDS), lanes]
                    for j in range(LOCAL):
                        sums[j] = sums[j] + x * weights[b, i * 8 + k, to, j : j + 1, lanes]
                return tuple(sums)

            sums = lax.fori_loop(
                0, MEMBERS // 8, step, tuple(jnp.zeros((FIELDS, 128), F32) for _ in range(LOCAL))
            )
            for j in range(LOCAL):
                value = (sums[j] + mean_of[b, :, lanes]).astype(BF16)

                @pl.when(s < 7)
                def _():
                    result[b, to, j * FIELDS : (j + 1) * FIELDS, lanes] = value

                @pl.when(s == 7)
                def _():
                    returned[b, m, j * FIELDS : (j + 1) * FIELDS, lanes] = value

        @pl.when(s < 3)
        def _():
            return_copy(to, b).start()

        @pl.when(s == 4)
        def _():
            start_pieces(result.at[b], returned.at[b], rt_send, rt_recv, (3, 4), b * 8)

        @pl.when(s == 6)
        def _():
            start_pieces(result.at[b], returned.at[b], rt_send, rt_recv, (5, 6), b * 8)

        return carry

    lax.fori_loop(0, 16, analyse, 0)

    total[...] = jnp.zeros((ROWS, PATCH), F32)

    def place(i, carry):
        s = (i + 7) % 8
        frm = turn(s, -1)
        first = (z - frm % 4 + 8) % 8
        second = (first + 4) % 8
        close = jnp.minimum(first, 8 - first) <= jnp.minimum(second, 8 - second)
        b = jnp.where(close, i // 8, 1 - i // 8)

        @pl.when(s < 7)
        def _():
            copy(
                result.at[b, frm], returned.at[b, frm], rt_send.at[b * 8 + frm],
                rt_recv.at[b * 8 + frm], frm, g,
            ).wait_recv()

        onehot_into(oh, hi_ref, half_ids(frm, b))
        for part_of in range(8):
            cells = slice(part_of * 512, (part_of + 1) * 512)
            total[:, cells] += lax.dot_general(
                returned[b, frm], oh[cells, 0:256], (((1,), (1,)), ((), ())),
                preferred_element_type=F32,
            )
        return carry

    lax.fori_loop(0, 16, place, 0)
    out_ref[...] = total[...].astype(BF16)

    for s in range(1, 8):
        z_copy(s).wait_send()
        state_copy((m + s) % 8).wait_send()
        for b in range(2):
            return_copy((m + s) % 8, b).wait_send()
    param_sends(lambda sent: sent.wait_send())
    core_copy.wait_send()
    for r in range(9):
        for b in range(2):
            c_copy(c, r, b).wait_send()

            @pl.when(passes_on[b])
            def _():
                t_copy(r, b, t_send, ahead[b]).wait_send()

            @pl.when(far[b] == 0)
            def _():
                t_copy(r, b, t_back, (z + 7) % 8).wait_send()

    @pl.when(jnp.logical_and(root, jnp.logical_not(native)))
    def _():
        for r in range(8):
            y_copy(r).wait_send()

    @pl.when(rim_across)
    def _():
        across.wait_send()

    @pl.when(rim_along)
    def _():
        along.wait_send()


def on_device(prior, mapping, triples, factors, transforms):
    mapping = jnp.transpose(mapping, (1, 2, 0))
    vmem = pl.BlockSpec(memory_space=pltpu.VMEM)
    dma = pltpu.SemaphoreType.DMA
    out = pl.pallas_call(
        kernel,
        out_shape=jax.ShapeDtypeStruct((ROWS, PATCH), BF16),
        in_specs=[vmem] * 5,
        out_specs=vmem,
        scratch_shapes=[
            pltpu.VMEM((GROUPS, 2, 2, POINTS), jnp.int32),
            pltpu.VMEM((4, HEAD, POINTS), BF16),
            pltpu.VMEM((4, 2, HEAD, POINTS), BF16),
            pltpu.VMEM((2, 8, 2, HEAD, POINTS), BF16),
            pltpu.VMEM((8, PAIRS, POINTS), BF16),
            pltpu.VMEM((2, 9, 2, PAIRS, POINTS), BF16),
            pltpu.VMEM((PAIRS, POINTS), BF16),
            pltpu.VMEM((8, ROWS, BLOCK), BF16),
            pltpu.VMEM((8, ROWS, BLOCK), BF16),
            pltpu.VMEM((FIELDS, BLOCK), F32),
            pltpu.VMEM((2, FIELDS, 256), F32),
            pltpu.VMEM((2, MEMBERS * FIELDS, 256), F32),
            pltpu.VMEM((2, MEMBERS, GROUPS, 8, 256), F32),
            pltpu.VMEM((2, 8, ROWS, 256), BF16),
            pltpu.VMEM((2, 8, ROWS, 256), BF16),
            pltpu.VMEM((ROWS, PATCH), F32),
            pltpu.VMEM((PATCH, BLOCK), BF16),
            pltpu.VMEM((64, BLOCK), F32),
            pltpu.VMEM((4, HEAD, POINTS), F32),
            pltpu.VMEM((2, 256, 256), BF16),
            pltpu.VMEM((2, POINTS, POINTS), BF16),
            dma((8,)), dma((8,)), dma((8,)), dma((8,)), dma((2,)), dma((1,)),
            dma((8,)), dma((18,)), dma((18,)), dma((18,)), dma((18,)), dma((18,)),
            dma((8,)), dma((8,)), dma((16,)), dma((16,)),
        ],
        compiler_params=pltpu.CompilerParams(
            collective_id=0, has_side_effects=True, vmem_limit_bytes=62 * 1024 * 1024
        ),
    )(
        prior.reshape(ROWS, PATCH), mapping, jnp.transpose(triples, (1, 0, 2)),
        jnp.transpose(factors, (1, 0, 2)), transforms,
    )
    return out.reshape(LOCAL, FIELDS, PATCH)


def solution(mesh):
    return jax.shard_map(
        on_device,
        mesh=mesh,
        in_specs=(
            P("member", None, "grid"),
            P(None, None, "grid"),
            P("grid", None, "member"),
            P("grid", None, "member"),
            P(None, "grid"),
        ),
        out_specs=P("member", None, "grid"),
        check_vma=False,
    )
```
